32 devices in a mesh: groups: 2 (over y), ctx: 4 (over x, core), head: 4 (over z).
Axes of the slice: x: 2, y: 2, z: 4, core: 2. Of those that a mesh axis runs over, the one named last changes fastest.
Arguments:
- queries: bfloat16 [384, 64, 128], P(('groups', 'ctx'), 'head'), parts along dimension 0, may hold values from -16 to 16
- prefix_keys: bfloat16 [16384, 8, 128], P(('groups', 'ctx'), 'head'), parts along dimension 0, may hold values from -16 to 16
- prefix_values: bfloat16 [16384, 8, 128], P(('groups', 'ctx'), 'head'), parts along dimension 0, may hold values from -12 to 12
- suffix_keys: bfloat16 [384, 512, 8, 128], P(('groups', 'ctx'), None, 'head'), parts along dimension 0, may hold values from -16 to 16
- suffix_values: bfloat16 [384, 512, 8, 128], P(('groups', 'ctx'), None, 'head'), parts along dimension 0, may hold values from -12 to 12
- lengths: int32 [384], P(('groups', 'ctx')), parts along dimension 0, may hold values from 1 to 512, as said below
Outputs:
- attended: bfloat16 [384, 64, 128], P(('groups', 'ctx'), 'head'), parts along dimension 0
The draws below stay inside these ranges and needn't reach their ends.
There are 2 independent parts, one for each index of `groups`. The reference program is written for one: setup_inputs(seed, part) draws one part's arguments, and reference() takes and returns one part's arrays. A program takes and returns all parts, laid end to end along the dimension named above; each array names one. Nothing has to cross between parts.
Inputs may be any that keep to these rules, and one draw needn't show every extreme that they name: The live slots of a row are its first lengths[r] slots; some row of each part has exactly 512.
All inputs are finite; a program needn't handle non-finite values.
Results may differ from the reference program's by a relative error of at most 0.0025.
Values may be sent and summed in bfloat16 or wider, within the bound.
A program may use at most 128 MiB of HBM per device.

```python
import math
import jax
import jax.numpy as jnp
from jax import lax

Q_HEADS = 64
KV_HEADS = 8
HEAD_DIM = 128
ROWS_DEV = 48
PREFIX_DEV = 2048
SUFFIX = 512
ROWS = 192
PREFIX = 8192
N_CTX = 4


def draw_queries(key, part):
    key_base = jax.random.fold_in(key, 1)
    base_draw = jnp.clip(jax.random.normal(key_base, (ROWS, Q_HEADS, HEAD_DIM), jnp.float32), -5.0, 5.0)
    return base_draw.astype(jnp.bfloat16)


def draw_prefix_keys(key, part):
    key_base = jax.random.fold_in(key, 2)
    base_draw = jnp.clip(2.5 * jax.random.normal(key_base, (PREFIX, KV_HEADS, HEAD_DIM), jnp.float32), -15.0, 15.0)
    return base_draw.astype(jnp.bfloat16)


def draw_lengths(key, part):
    key_level, key_raw, key_long = jax.random.split(jax.random.fold_in(key, 5), 3)
    block_count = ROWS // ROWS_DEV
    levels = jax.random.randint(key_level, (block_count,), 1, 9)
    ceiling = jnp.repeat(SUFFIX * levels // 8, ROWS_DEV, total_repeat_length=ROWS)
    raw_draw = jax.random.randint(key_raw, (ROWS,), 0, SUFFIX)
    result = 1 + raw_draw % ceiling
    longest = jax.random.randint(key_long, (), 0, ROWS)
    result = result.at[longest].set(SUFFIX)
    return result.astype(jnp.int32)


def block_levels(rng, shape, cuts, low, high):
    loudness = 1.0
    for position, shards_of in cuts:
        draws = jax.random.uniform(jax.random.fold_in(jax.random.fold_in(rng, 6), position), (shards_of,), jnp.float32, low / len(cuts), high / len(cuts))
        loudness = loudness * jnp.repeat(jnp.exp(draws), shape[position] // shards_of).reshape((-1,) + (1,) * (len(shape) - 1 - position))
    return loudness


def normal_values(stream_key, dims, deviation, limit, cuts=(), kind=jnp.bfloat16):
    array = jax.random.normal(stream_key, dims, jnp.float32) * deviation
    if len(cuts) > 0:
        array = block_levels(stream_key, dims, cuts, -0.22, 0.18) * array
    return jnp.clip(array, min=-limit, max=limit).astype(kind)


def setup_inputs(seed: int = 0, part: int = 0) -> dict:
    streams_of = jax.random.split(jax.random.key(seed), 7)
    part_splits = jax.random.split(jax.random.fold_in(streams_of[6], part), 7)
    queries = draw_queries(jax.random.fold_in(jax.random.fold_in(streams_of[6], part), 71), part)
    prefix_keys = draw_prefix_keys(jax.random.fold_in(jax.random.fold_in(streams_of[6], part), 71), part)
    prefix_values = normal_values(part_splits[2], (PREFIX, KV_HEADS, HEAD_DIM), 2.0, 12.0, ((0, 4), (1, 4)))
    suffix_keys = normal_values(part_splits[3], (ROWS, SUFFIX, KV_HEADS, HEAD_DIM), 4.0, 16.0, ((0, 4), (2, 4)))
    suffix_values = normal_values(part_splits[4], (ROWS, SUFFIX, KV_HEADS, HEAD_DIM), 2.0, 12.0, ((0, 4), (2, 4)))
    lengths = draw_lengths(jax.random.fold_in(jax.random.fold_in(streams_of[6], part), 71), part)
    return {"queries": queries, "prefix_keys": prefix_keys, "prefix_values": prefix_values, "suffix_keys": suffix_keys, "suffix_values": suffix_values, "lengths": lengths}


def reference(queries, prefix_keys, prefix_values, suffix_keys, suffix_values, lengths):
    rows, heads, head_width = queries.shape
    kv_count = prefix_keys.shape[1]
    group_size = heads // kv_count
    span = suffix_keys.shape[1]
    scaling = head_width ** -0.5
    keys_wide = prefix_keys.astype(jnp.float32)
    values_wide = prefix_values.astype(jnp.float32).reshape(N_CTX, PREFIX_DEV, kv_count, head_width)
    positions = jnp.arange(span, dtype=jnp.int32)
    block_rows = math.gcd(rows, 8)
    count_blocks = rows // block_rows

    def one_block(pieces):
        query_block, keys_block, values_block, length_block = pieces
        grouped = query_block.astype(jnp.float32).reshape(block_rows, kv_count, group_size, head_width)
        prefix_part = jnp.einsum("rkgd,pkd->rkgp", grouped, keys_wide, precision=lax.Precision.HIGHEST) * scaling
        prefix_part = prefix_part.reshape(block_rows, kv_count, group_size, N_CTX, PREFIX_DEV)
        suffix_part = jnp.einsum("rkgd,rskd->rkgs", grouped, keys_block.astype(jnp.float32), precision=lax.Precision.HIGHEST) * scaling
        live_mask = (positions[None, :] < length_block[:, None])[:, None, None, :]
        block_top = jnp.max(prefix_part, axis=-1)
        row_top = jnp.maximum(jnp.max(block_top, axis=-1), jnp.max(jnp.where(live_mask, suffix_part, -jnp.inf), axis=-1))
        prefix_weights = jnp.exp(prefix_part - block_top[..., None]).astype(jnp.bfloat16)
        block_scale = jnp.exp(block_top - row_top[..., None])
        suffix_weights = jnp.where(live_mask, jnp.exp(suffix_part - row_top[..., None]), 0.0).astype(jnp.bfloat16)
        prefix_float = prefix_weights.astype(jnp.float32)
        suffix_float = suffix_weights.astype(jnp.float32)
        weight_sum = jnp.sum(jnp.sum(prefix_float, axis=-1) * block_scale, axis=-1) + jnp.sum(suffix_float, axis=-1)
        partial_accum = jnp.einsum("rkgcp,cpkd->rkgcd", prefix_float, values_wide, precision=lax.Precision.HIGHEST)
        accumulated = jnp.sum(partial_accum * block_scale[..., None], axis=-2)
        accumulated = accumulated + jnp.einsum("rkgs,rskd->rkgd", suffix_float, values_block.astype(jnp.float32), precision=lax.Precision.HIGHEST)
        result = (accumulated / weight_sum[..., None]).astype(jnp.bfloat16)
        return result.reshape(block_rows, heads, head_width)

    stacked = lax.map(one_block, (
        queries.reshape(count_blocks, block_rows, heads, head_width),
        suffix_keys.reshape(count_blocks, block_rows, span, kv_count, head_width),
        suffix_values.reshape(count_blocks, block_rows, span, kv_count, head_width),
        lengths.reshape(count_blocks, block_rows)))
    return stacked.reshape(rows, heads, head_width)
```

```python
import functools
import math

import jax
import jax.numpy as jnp
from jax import lax
from jax.experimental import pallas as pl
from jax.experimental.pallas import tpu as pltpu
from jax.sharding import PartitionSpec as P

F32 = jnp.float32
BF16 = jnp.bfloat16
MASKED = -1e30
LANES = 128


def dot_t(a, b):
    return lax.dot_general(a, b, (((1,), (1,)), ((), ())), preferred_element_type=F32)


def kernel(
    n_ctx, tile_rows, first_tiles,
    len_ref, q_hbm, pk_hbm, pv_hbm, sk_hbm, sv_hbm, out_ref,
    q_raw, qk, k_raw, v_raw, k_cut, v_cut, wide, sk, sv,
    part_acc, part_stat, got_acc, got_stat,
    own_acc, own_top, own_sum, suf_acc, suf_top, suf_sum,
    q_sem, kv_sem, suf_sem, q_send, q_recv, kv_send, kv_recv, p_send, p_recv,
):
    rows, heads, width = q_hbm.shape
    kv = k_cut.shape[1]
    group = heads // kv
    flat = rows * group
    pair = 2 if n_ctx % 2 == 0 else 1
    chips = n_ctx // pair
    blocks = pair
    factor = width ** (-0.5) * math.log2(math.e)
    tiles = rows // tile_rows
    slots = sk.shape[1]
    me = lax.axis_index("ctx")
    chip, core = me // pair, me % pair

    def device(chip_at, core_at):
        return {"ctx": chip_at * pair + core_at}

    def remote(src, dst, send, recv, target):
        return pltpu.make_async_remote_copy(
            src_ref=src, dst_ref=dst, send_sem=send, recv_sem=recv,
            device_id=target, device_id_type=pl.DeviceIdType.MESH,
        )

    q_copy = pltpu.make_async_copy(q_hbm, q_raw.at[0], q_sem)
    q_copy.start()
    kv_copies = [
        pltpu.make_async_copy(pk_hbm, k_raw.at[0], kv_sem.at[0]),
        pltpu.make_async_copy(pv_hbm, v_raw.at[0], kv_sem.at[1]),
    ]
    for copy in kv_copies:
        copy.start()

    def suffix_copies(tile):
        span = pl.ds(tile * tile_rows, tile_rows)
        return (
            pltpu.make_async_copy(sk_hbm.at[span], sk.at[span], suf_sem.at[tile, 0]),
            pltpu.make_async_copy(sv_hbm.at[span], sv.at[span], suf_sem.at[tile, 1]),
        )

    partners = [device(lax.rem(chip + t, chips), core) for t in range(1, chips)]
    backs = [device(lax.rem(chip - t + chips, chips), core) for t in range(1, chips)]
    twin = device(chip, pair - 1 - core)
    greeted = partners + ([twin] if pair == 2 else [])
    if greeted:
        barrier = pltpu.get_barrier_semaphore()
        for target in greeted:
            pl.semaphore_signal(
                barrier, inc=1, device_id=target, device_id_type=pl.DeviceIdType.MESH
            )
        pl.semaphore_wait(barrier, len(greeted))

    q_sends = [
        remote(q_hbm, q_raw.at[t + 1], q_send.at[t], q_recv.at[t], partners[t])
        for t in range(chips - 1)
    ]
    for copy in q_sends:
        copy.start()
    kv_sends = []
    if pair == 2:
        kv_sends = [
            remote(pk_hbm, k_raw.at[1], kv_send.at[0], kv_recv.at[0], twin),
            remote(pv_hbm, v_raw.at[1], kv_send.at[1], kv_recv.at[1], twin),
        ]
        for copy in kv_sends:
            copy.start()

    def start_tile(tile, carry):
        for copy in suffix_copies(tile):
            copy.start()
        return carry

    lax.fori_loop(0, tiles, start_tile, 0)

    def split_queries(slot):
        wide_q = q_raw[slot].astype(F32).reshape(rows, kv, group, width)
        for k in range(kv):
            qk[slot, k] = wide_q[:, k].reshape(flat, width).astype(BF16)

    span = k_cut.shape[2]
    piece = wide.shape[1]
    pieces = span * kv // piece

    def split_block(block):
        def step(i, carry):
            at = pl.ds(pl.multiple_of(i * piece, piece), piece)
            to = pl.ds(pl.multiple_of(i * (piece // kv), piece // kv), piece // kv)
            wide[0] = k_raw[block, at, :].astype(F32)
            wide[1] = v_raw[block, at, :].astype(F32)
            for k in range(kv):
                rows_k = pl.ds(k, piece // kv, stride=kv) if kv > 1 else pl.ds(0, piece)
                k_cut[block, k, to, :] = wide[0, rows_k, :].astype(BF16)
                v_cut[block, k, to, 0:width] = wide[1, rows_k, :].astype(BF16)
                v_cut[block, k, to, width : 2 * width] = jnp.ones((piece // kv, width), BF16)
            return carry

        lax.fori_loop(0, pieces, step, 0)

    step_rows = LANES
    chunks = flat // step_rows

    def block_terms(slot, k, block):
        scores = dot_t(qk[slot, k], k_cut[block, k])
        top = jnp.max(scores, axis=1, keepdims=True)
        weights = jnp.exp2((scores - top) * factor).astype(BF16)
        both = jnp.dot(weights, v_cut[block, k], preferred_element_type=F32)
        return top * factor, both[:, :width], both[:, width:]

    def merge(one, two):
        top = jnp.maximum(one[0], two[0])
        a, b = jnp.exp2(one[0] - top), jnp.exp2(two[0] - top)
        return top, one[1] * a + two[1] * b, one[2] * a + two[2] * b

    def own_block(block):
        def step(k, carry):
            terms = block_terms(0, k, block)
            if block > 0:
                terms = merge(terms, (own_top[k], own_acc[k], own_sum[k]))
            own_top[k] = jnp.broadcast_to(terms[0], (flat, width))
            own_acc[k] = terms[1]
            own_sum[k] = terms[2]
            return carry

        lax.fori_loop(0, kv, step, 0)

    diagonal = lax.broadcasted_iota(jnp.int32, (step_rows, LANES), 0) == lax.broadcasted_iota(
        jnp.int32, (step_rows, LANES), 1
    )

    def partial_copies(t, k):
        return (
            remote(part_acc.at[t, k], got_acc.at[t, k], p_send.at[t, k, 0], p_recv.at[t, k, 0], backs[t]),
            remote(part_stat.at[t, k], got_stat.at[t, k], p_send.at[t, k, 1], p_recv.at[t, k, 1], backs[t]),
        )

    def remote_rows(t):
        for k in range(kv):
            terms = block_terms(t + 1, k, 0)
            for block in range(1, blocks):
                terms = merge(terms, block_terms(t + 1, k, block))
            part_acc[t, k] = terms[1]
            top_wide = jnp.broadcast_to(terms[0], (flat, LANES))
            for c in range(chunks):
                at = slice(c * step_rows, (c + 1) * step_rows)
                for i, x in enumerate((top_wide, terms[2])):
                    row = 2 * c + i
                    part_stat[t, k, row : row + 1, :] = jnp.sum(
                        jnp.where(diagonal, x[at], 0.0), axis=0, keepdims=True
                    )
            for copy in partial_copies(t, k):
                copy.start()

    column = lax.broadcasted_iota(jnp.int32, (heads, slots), 1)
    same_head = column % kv == lax.broadcasted_iota(jnp.int32, (heads, slots), 0) // group
    nothing = jnp.zeros((heads, width), BF16)

    def suffix_pair(r):
        ask = jnp.concatenate(
            [
                jnp.concatenate([q_raw[0, r], nothing], axis=1),
                jnp.concatenate([nothing, q_raw[0, r + 1]], axis=1),
            ],
            axis=0,
        )
        both = dot_t(ask, jnp.concatenate([sk[r], sk[r + 1]], axis=1))
        done = []
        for i in range(2):
            live = same_head & (column < len_ref[r + i] * kv)
            scores = jnp.where(live, both[i * heads : (i + 1) * heads], MASKED)
            top = jnp.max(scores, axis=1, keepdims=True)
            weights = jnp.exp2((scores - top) * factor).astype(BF16)
            total = jnp.sum(weights.astype(F32), axis=1, keepdims=True)
            done.append((top * factor, weights, total))
        joined = jnp.concatenate([x[1] for x in done], axis=0)
        out = jnp.dot(
            joined, jnp.concatenate([sv[r], sv[r + 1]], axis=1), preferred_element_type=F32
        )
        for i in range(2):
            acc = out[i * heads : (i + 1) * heads, i * width : (i + 1) * width]
            top = jnp.broadcast_to(done[i][0], (heads, width))
            total = jnp.broadcast_to(done[i][2], (heads, width))
            to = pl.ds(pl.multiple_of((r + i) * group, group), group)
            for k in range(kv):
                part = slice(k * group, (k + 1) * group)
                suf_acc[k, to, :] = acc[part]
                suf_top[k, to, :] = top[part]
                suf_sum[k, to, :] = total[part]

    def suffix_tile(tile, carry):
        for copy in suffix_copies(tile):
            copy.wait()
        for i in range(0, tile_rows, 2):
            suffix_pair(tile * tile_rows + i)
        return carry

    q_copy.wait()
    split_queries(0)
    for copy in kv_copies:
        copy.wait()
    split_block(0)
    own_block(0)
    lax.fori_loop(0, first_tiles, suffix_tile, 0)
    for copy in kv_sends:
        copy.wait_recv()
    for block in range(1, blocks):
        split_block(block)
    for t in range(chips - 1):
        q_sends[t].wait_recv()
        split_queries(t + 1)
        remote_rows(t)
    for block in range(1, blocks):
        own_block(block)
    lax.fori_loop(first_tiles, tiles, suffix_tile, 0)

    for k in range(kv):
        for t in range(chips - 1):
            for copy in partial_copies(t, k):
                copy.wait_recv()
    per = step_rows // group
    for c in range(chunks):
        at = pl.ds(c * step_rows, step_rows)
        done = []
        for k in range(kv):
            terms = merge(
                (own_top[k, at, :], own_acc[k, at, :], own_sum[k, at, :]),
                (suf_top[k, at, :], suf_acc[k, at, :], suf_sum[k, at, :]),
            )
            for t in range(chips - 1):
                stats = []
                for i in range(2):
                    row = jnp.broadcast_to(
                        got_stat[t, k, 2 * c + i : 2 * c + i + 1, :], (step_rows, LANES)
                    )
                    stats.append(jnp.sum(jnp.where(diagonal, row, 0.0), axis=1, keepdims=True))
                terms = merge(terms, (stats[0], got_acc[t, k, at, :], stats[1]))
            done.append((terms[1] / terms[2]).reshape(per, 1, group, width))
        joined = jnp.concatenate(done, axis=1).reshape(per, heads, width)
        out_ref[c * per : (c + 1) * per] = joined.astype(BF16)
    for copy in q_sends + kv_sends:
        copy.wait_send()
    for t in range(chips - 1):
        for k in range(kv):
            for copy in partial_copies(t, k):
                copy.wait_send()


def shards(n_ctx, queries, prefix_keys, prefix_values, suffix_keys, suffix_values, lengths):
    rows, heads, width = queries.shape
    positions, kv, _ = prefix_keys.shape
    slots = suffix_keys.shape[1] * kv
    flat = rows * (heads // kv)
    pair = 2 if n_ctx % 2 == 0 else 1
    others = max(1, n_ctx // pair - 1)
    tile_rows = math.gcd(rows, 8)
    tiles = rows // tile_rows
    first_tiles = tiles // 3
    stat_rows = -(-2 * (flat // LANES) // 8) * 8
    piece = math.gcd(positions * kv, 1024)
    anywhere = pl.BlockSpec(memory_space=pl.ANY)
    vmem = pltpu.VMEM
    dma = pltpu.SemaphoreType.DMA
    call = pl.pallas_call(
        functools.partial(kernel, n_ctx, tile_rows, first_tiles),
        out_shape=jax.ShapeDtypeStruct((rows, heads, width), BF16),
        in_specs=[pl.BlockSpec(memory_space=pltpu.SMEM)] + [anywhere] * 5,
        out_specs=pl.BlockSpec(memory_space=vmem),
        scratch_shapes=[
            vmem((1 + others, rows, heads, width), BF16),
            vmem((1 + others, kv, flat, width), BF16),
            vmem((pair, positions * kv, width), BF16),
            vmem((pair, positions * kv, width), BF16),
            vmem((pair, kv, positions, width), BF16),
            vmem((pair, kv, positions, 2 * width), BF16),
            vmem((2, piece, width), F32),
            vmem((rows, slots, width), BF16),
            vmem((rows, slots, width), BF16),
            vmem((others, kv, flat, width), F32),
            vmem((others, kv, stat_rows, LANES), F32),
            vmem((others, kv, flat, width), F32),
            vmem((others, kv, stat_rows, LANES), F32),
        ]
        + [vmem((kv, flat, width), F32)] * 6
        + [
            dma,
            dma((2,)),
            dma((tiles, 2)),
            dma((others,)),
            dma((others,)),
            dma((2,)),
            dma((2,)),
            dma((others, kv, 2)),
            dma((others, kv, 2)),
        ],
        compiler_params=pltpu.CompilerParams(
            collective_id=0, has_side_effects=True, vmem_limit_bytes=62 * 1024 * 1024
        ),
    )
    return call(
        lengths,
        queries,
        prefix_keys.reshape(positions * kv, width),
        prefix_values.reshape(positions * kv, width),
        suffix_keys.reshape(rows, slots, width),
        suffix_values.reshape(rows, slots, width),
    )


def solution(mesh):
    placed = (
        P(("groups", "ctx"), "head", None),
        P(("groups", "ctx"), "head", None),
        P(("groups", "ctx"), "head", None),
        P(("groups", "ctx"), None, "head", None),
        P(("groups", "ctx"), None, "head", None),
        P(("groups", "ctx")),
    )
    return jax.shard_map(
        functools.partial(shards, mesh.shape["ctx"]),
        mesh=mesh,
        in_specs=placed,
        out_specs=P(("groups", "ctx"), "head", None),
        check_vma=False,
    )
```

```python
import functools
import math

import jax
import jax.numpy as jnp
from jax import lax
from jax.experimental import pallas as pl
from jax.experimental.pallas import tpu as pltpu
from jax.sharding import PartitionSpec as P

F32 = jnp.float32
BF16 = jnp.bfloat16
MASKED = -1e30
LANES = 128


def dot_t(a, b):
    return lax.dot_general(a, b, (((1,), (1,)), ((), ())), preferred_element_type=F32)


def kernel(
    n_ctx, tile_rows, first_tiles,
    len_ref, q_hbm, pk_hbm, pv_hbm, sk_hbm, sv_hbm, out_ref,
    q_raw, qk, k_raw, v_raw, k_cut, v_turn, wide, sk, sv,
    scores_a, scores_b, weights_a, weights_b, top_a, top_b,
    acc_all, top_all, part, got, suf_acc, suf_top, suf_sum,
    q_sem, kv_sem, suf_sem, q_send, q_recv, kv_send, kv_recv, p_send, p_recv,
):
    rows, heads, width = q_hbm.shape
    kv = k_cut.shape[1]
    group = heads // kv
    flat = rows * group
    pair = 2 if n_ctx % 2 == 0 else 1
    chips = n_ctx // pair
    blocks = pair
    factor = width ** (-0.5) * math.log2(math.e)
    tiles = rows // tile_rows
    slots = sk.shape[1]
    span = k_cut.shape[2]
    tall = v_turn.shape[2]
    columns = scores_a.shape[1]
    me = lax.axis_index("ctx")
    chip, core = me // pair, me % pair

    def device(chip_at, core_at):
        return {"ctx": chip_at * pair + core_at}

    def remote(src, dst, send, recv, target):
        return pltpu.make_async_remote_copy(
            src_ref=src, dst_ref=dst, send_sem=send, recv_sem=recv,
            device_id=target, device_id_type=pl.DeviceIdType.MESH,
        )

    q_copy = pltpu.make_async_copy(q_hbm, q_raw.at[0], q_sem)
    q_copy.start()
    kv_copies = [
        pltpu.make_async_copy(pk_hbm, k_raw, kv_sem.at[0]),
        pltpu.make_async_copy(pv_hbm, v_raw, kv_sem.at[1]),
    ]
    for copy in kv_copies:
        copy.start()

    def suffix_copies(tile):
        at = pl.ds(tile * tile_rows, tile_rows)
        return (
            pltpu.make_async_copy(sk_hbm.at[at], sk.at[at], suf_sem.at[tile, 0]),
            pltpu.make_async_copy(sv_hbm.at[at], sv.at[at], suf_sem.at[tile, 1]),
        )

    partners = [device(lax.rem(chip + t, chips), core) for t in range(1, chips)]
    backs = [device(lax.rem(chip - t + chips, chips), core) for t in range(1, chips)]
    twin = device(chip, pair - 1 - core)
    greeted = partners + ([twin] if pair == 2 else [])
    if greeted:
        barrier = pltpu.get_barrier_semaphore()
        for target in greeted:
            pl.semaphore_signal(
                barrier, inc=1, device_id=target, device_id_type=pl.DeviceIdType.MESH
            )
        pl.semaphore_wait(barrier, len(greeted))

    q_sends = [
        remote(q_hbm, q_raw.at[t + 1], q_send.at[t], q_recv.at[t], partners[t])
        for t in range(chips - 1)
    ]
    for copy in q_sends:
        copy.start()

    def start_tile(tile, carry):
        for copy in suffix_copies(tile):
            copy.start()
        return carry

    lax.fori_loop(0, tiles, start_tile, 0)

    def split_queries(slot):
        wide_q = q_raw[slot].astype(F32).reshape(rows, kv, group, width)
        for k in range(kv):
            qk[k, slot * flat : (slot + 1) * flat] = wide_q[:, k].reshape(flat, width).astype(BF16)

    piece = wide.shape[1]
    cut = piece // kv

    def rows_of(k):
        return pl.ds(k, cut, stride=kv) if kv > 1 else pl.ds(0, piece)

    def split_keys():
        def step(i, carry):
            wide[0] = k_raw[pl.ds(pl.multiple_of(i * piece, piece), piece), :].astype(F32)
            to = pl.ds(pl.multiple_of(i * cut, cut), cut)
            for k in range(kv):
                k_cut[0, k, to, :] = wide[0, rows_of(k), :].astype(BF16)
            return carry

        lax.fori_loop(0, span * kv // piece, step, 0)

    def turn_values():
        ones = (lax.broadcasted_iota(jnp.int32, (tall - width, span), 0) == 0).astype(F32)
        for k in range(kv):
            v_turn[0, k, width:tall, :] = ones.astype(BF16)
        for i in range(span * kv // piece):
            wide[1] = v_raw[i * piece : (i + 1) * piece, :].astype(F32)
            for k in range(kv):
                turned = jnp.transpose(wide[1, rows_of(k), :])
                v_turn[0, k, 0:width, i * cut : (i + 1) * cut] = turned.astype(BF16)

    def kv_sends(k):
        if pair == 1:
            return []
        return [
            remote(k_cut.at[0, k], k_cut.at[1, k], kv_send.at[k, 0], kv_recv.at[k, 0], twin),
            remote(v_turn.at[0, k], v_turn.at[1, k], kv_send.at[k, 1], kv_recv.at[k, 1], twin),
        ]

    def merge(one, two):
        top = jnp.maximum(one[0], two[0])
        a, b = jnp.exp2(one[0] - top), jnp.exp2(two[0] - top)
        return top, one[1] * a + two[1] * b, one[2] * a + two[2] * b

    buffers = ((scores_a, weights_a, top_a), (scores_b, weights_b, top_b))
    height = math.gcd(span, 256)

    def unit_scores(unit, at):
        block, k, tile = unit
        scores, _, tops = buffers[at]
        ask = qk[k, tile * columns : (tile + 1) * columns]
        top = None
        for j in range(span // height):
            part_of = slice(j * height, (j + 1) * height)
            x = dot_t(k_cut[block, k, part_of], ask)
            scores[part_of] = x
            x = jnp.max(x.reshape(height // 8, 8, columns), axis=0)
            top = x if top is None else jnp.maximum(top, x)
        tops[...] = jnp.broadcast_to(jnp.max(top, axis=0, keepdims=True), (8, columns))

    def unit_sums(unit, at):
        block, k, tile = unit
        scores, weights, tops = buffers[at]
        for j in range(span // height):
            part_of = slice(j * height, (j + 1) * height)
            x = scores[part_of].reshape(height // 8, 8, columns)
            x = jnp.exp2((x - tops[...][None]) * factor)
            weights[part_of] = x.reshape(height, columns).astype(BF16)
        out = jnp.dot(v_turn[block, k], weights[...], preferred_element_type=F32)
        top = tops[...] * factor
        to = slice(tile * columns, (tile + 1) * columns)
        if block > 0:
            old = top_all[k, :, to]
            new = jnp.maximum(old, top)
            a, b = jnp.exp2(old - new), jnp.exp2(top - new)
            out = acc_all[k, :, to] * a[0:1] + out * b[0:1]
            top = new
        if block < blocks - 1:
            acc_all[k, :, to] = out
            top_all[k, :, to] = top
            return
        first = lax.broadcasted_iota(jnp.int32, (8, LANES), 0) == 0
        for c in range(columns // LANES):
            at_c = tile * columns + c * LANES
            here = slice(c * LANES, (c + 1) * LANES)
            slot, within = at_c // flat, at_c % flat
            if slot == 0:
                acc_all[k, :, at_c : at_c + LANES] = out[:, here]
                top_all[k, :, at_c : at_c + LANES] = top[:, here]
            else:
                into = slice(within, within + LANES)
                part[slot - 1, k, 0:width, into] = out[0:width, here]
                part[slot - 1, k, width : width + 8, into] = jnp.where(
                    first, out[width : width + 8, here], top[:, here]
                )

    def partial_copy(t, k):
        return remote(part.at[t, k], got.at[t, k], p_send.at[t, k], p_recv.at[t, k], backs[t])

    def run_units(steps):
        steps = list(steps)
        for i, (before, unit, after) in enumerate(steps):
            if i == 0:
                before()
                unit_scores(unit, 0)
            if i + 1 < len(steps):
                steps[i + 1][0]()
                unit_scores(steps[i + 1][1], (i + 1) % 2)
            unit_sums(unit, i % 2)
            after()

    def nop():
        pass

    column = lax.broadcasted_iota(jnp.int32, (heads, slots), 1)
    same_head = column % kv == lax.broadcasted_iota(jnp.int32, (heads, slots), 0) // group
    nothing = jnp.zeros((heads, width), BF16)

    def suffix_pair(r):
        ask = jnp.concatenate(
            [
                jnp.concatenate([q_raw[0, r], nothing], axis=1),
                jnp.concatenate([nothing, q_raw[0, r + 1]], axis=1),
            ],
            axis=0,
        )
        both = dot_t(ask, jnp.concatenate([sk[r], sk[r + 1]], axis=1))
        done = []
        for i in range(2):
            live = same_head & (column < len_ref[r + i] * kv)
            scores = jnp.where(live, both[i * heads : (i + 1) * heads], MASKED)
            top = jnp.max(scores, axis=1, keepdims=True)
            weights = jnp.exp2((scores - top) * factor).astype(BF16)
            total = jnp.sum(weights.astype(F32), axis=1, keepdims=True)
            done.append((top * factor, weights, total))
        joined = jnp.concatenate([x[1] for x in done], axis=0)
        out = jnp.dot(
            joined, jnp.concatenate([sv[r], sv[r + 1]], axis=1), preferred_element_type=F32
        )
        for i in range(2):
            acc = out[i * heads : (i + 1) * heads, i * width : (i + 1) * width]
            top = jnp.broadcast_to(done[i][0], (heads, width))
            total = jnp.broadcast_to(done[i][2], (heads, width))
            to = pl.ds(pl.multiple_of((r + i) * group, group), group)
            for k in range(kv):
                part = slice(k * group, (k + 1) * group)
                suf_acc[k, to, :] = acc[part]
                suf_top[k, to, :] = top[part]
                suf_sum[k, to, :] = total[part]

    def suffix_tile(tile, carry):
        for copy in suffix_copies(tile):
            copy.wait()
        for i in range(0, tile_rows, 2):
            suffix_pair(tile * tile_rows + i)
        return carry

    all_tiles = chips * flat // columns
    near = flat // columns

    q_copy.wait()
    split_queries(0)
    kv_copies[0].wait()
    split_keys()
    kv_copies[1].wait()
    turn_values()
    for k in range(kv):
        for copy in kv_sends(k):
            copy.start()
    run_units([(nop, (0, k, tile), nop) for tile in range(near) for k in range(kv)])
    lax.fori_loop(0, first_tiles, suffix_tile, 0)

    waited = set()

    def ready(block, k, tile):
        def go():
            last = ((tile + 1) * columns - 1) // flat
            for t in range(last):
                if ("q", t) not in waited:
                    waited.add(("q", t))
                    q_sends[t].wait_recv()
                    split_queries(t + 1)
            if block > 0 and ("kv", k) not in waited:
                waited.add(("kv", k))
                for copy in kv_sends(k):
                    copy.wait_recv()

        return go

    def finish(block, k, tile):
        def go():
            if block == blocks - 1:
                for t in range(chips - 1):
                    end = (t + 2) * flat
                    if tile * columns < end <= (tile + 1) * columns:
                        partial_copy(t, k).start()

        return go

    order = [
        (block, k, tile) for k in range(kv) for tile in range(near, all_tiles) for block in range(blocks)
    ] + [(block, k, tile) for k in range(kv) for tile in range(near) for block in range(1, blocks)]
    run_units([(ready(*unit), unit, finish(*unit)) for unit in order])
    lax.fori_loop(first_tiles, tiles, suffix_tile, 0)

    for k in range(kv):
        for t in range(chips - 1):
            partial_copy(t, k).wait_recv()
    diagonal = lax.broadcasted_iota(jnp.int32, (LANES, LANES), 0) == lax.broadcasted_iota(
        jnp.int32, (LANES, LANES), 1
    )

    def upright(row):
        wide_row = jnp.broadcast_to(row, (LANES, LANES))
        return jnp.sum(jnp.where(diagonal, wide_row, 0.0), axis=1, keepdims=True)

    per = LANES // group
    for c in range(flat // LANES):
        at = slice(c * LANES, (c + 1) * LANES)
        done = []
        for k in range(kv):
            terms = (
                top_all[k, 0:1, at],
                acc_all[k, 0:width, at],
                acc_all[k, width : width + 1, at],
            )
            for t in range(chips - 1):
                terms = merge(
                    terms,
                    (
                        got[t, k, width + 1 : width + 2, at],
                        got[t, k, 0:width, at],
                        got[t, k, width : width + 1, at],
                    ),
                )
            terms = merge(
                (upright(terms[0]), jnp.transpose(terms[1]), upright(terms[2])),
                (suf_top[k, at, :], suf_acc[k, at, :], suf_sum[k, at, :]),
            )
            done.append((terms[1] / terms[2]).reshape(per, 1, group, width))
        joined = jnp.concatenate(done, axis=1).reshape(per, heads, width)
        out_ref[c * per : (c + 1) * per] = joined.astype(BF16)
    for copy in q_sends:
        copy.wait_send()
    for k in range(kv):
        for copy in kv_sends(k):
            copy.wait_send()
        for t in range(chips - 1):
            partial_copy(t, k).wait_send()


def shards(n_ctx, queries, prefix_keys, prefix_values, suffix_keys, suffix_values, lengths):
    rows, heads, width = queries.shape
    positions, kv, _ = prefix_keys.shape
    slots = suffix_keys.shape[1] * kv
    flat = rows * (heads // kv)
    pair = 2 if n_ctx % 2 == 0 else 1
    others = max(1, n_ctx // pair - 1)
    tile_rows = math.gcd(rows, 8)
    tiles = rows // tile_rows
    first_tiles = tiles // 3
    columns = math.gcd(n_ctx // pair * flat, 256)
    tall = width + 16
    piece = math.gcd(positions * kv, 1024)
    anywhere = pl.BlockSpec(memory_space=pl.ANY)
    vmem = pltpu.VMEM
    dma = pltpu.SemaphoreType.DMA
    call = pl.pallas_call(
        functools.partial(kernel, n_ctx, tile_rows, first_tiles),
        out_shape=jax.ShapeDtypeStruct((rows, heads, width), BF16),
        in_specs=[pl.BlockSpec(memory_space=pltpu.SMEM)] + [anywhere] * 5,
        out_specs=pl.BlockSpec(memory_space=vmem),
        scratch_shapes=[
            vmem((1 + others, rows, heads, width), BF16),
            vmem((kv, n_ctx // pair * flat, width), BF16),
            vmem((positions * kv, width), BF16),
            vmem((positions * kv, width), BF16),
            vmem((pair, kv, positions, width), BF16),
            vmem((pair, kv, tall, positions), BF16),
            vmem((2, piece, width), F32),
            vmem((rows, slots, width), BF16),
            vmem((rows, slots, width), BF16),
            vmem((positions, columns), F32),
            vmem((positions, columns), F32),
            vmem((positions, columns), BF16),
            vmem((positions, columns), BF16),
            vmem((8, columns), F32),
            vmem((8, columns), F32),
            vmem((kv, tall, n_ctx // pair * flat), F32),
            vmem((kv, 8, n_ctx // pair * flat), F32),
            vmem((others, kv, width + 8, flat), F32),
            vmem((others, kv, width + 8, flat), F32),
        ]
        + [vmem((kv, flat, width), F32)] * 3
        + [
            dma,
            dma((2,)),
            dma((tiles, 2)),
            dma((others,)),
            dma((others,)),
            dma((kv, 2)),
            dma((kv, 2)),
            dma((others, kv)),
            dma((others, kv)),
        ],
        compiler_params=pltpu.CompilerParams(
            collective_id=0, has_side_effects=True, vmem_limit_bytes=62 * 1024 * 1024
        ),
    )
    return call(
        lengths,
        queries,
        prefix_keys.reshape(positions * kv, width),
        prefix_values.reshape(positions * kv, width),
        suffix_keys.reshape(rows, slots, width),
        suffix_values.reshape(rows, slots, width),
    )


def solution(mesh):
    placed = (
        P(("groups", "ctx"), "head", None),
        P(("groups", "ctx"), "head", None),
        P(("groups", "ctx"), "head", None),
        P(("groups", "ctx"), None, "head", None),
        P(("groups", "ctx"), None, "head", None),
        P(("groups", "ctx")),
    )
    return jax.shard_map(
        functools.partial(shards, mesh.shape["ctx"]),
        mesh=mesh,
        in_specs=placed,
        out_specs=P(("groups", "ctx"), "head", None),
        check_vma=False,
    )
```

```python
import functools
import math

import jax
import jax.numpy as jnp
from jax import lax
from jax.experimental import pallas as pl
from jax.experimental.pallas import tpu as pltpu
from jax.sharding import PartitionSpec as P

F32 = jnp.float32
BF16 = jnp.bfloat16
MASKED = -1e30
LANES = 128


def dot_t(a, b):
    return lax.dot_general(a, b, (((1,), (1,)), ((), ())), preferred_element_type=F32)


def kernel(
    n_ctx, tile_rows,
    len_ref, q_hbm, pk_hbm, pv_hbm, sk_hbm, sv_hbm, out_ref,
    q_raw, qk, k_raw, v_raw, k_cut, v_turn, wide, sk, sv,
    scores_a, scores_b, weights_a, weights_b, top_a, top_b,
    ask_a, ask_b, near_a, near_b, far_a, far_b, acc_all, top_all, part, got, q_turn, suf_acc, suf_top, suf_sum,
    q_sem, kv_sem, suf_sem, q_send, q_recv, kv_send, kv_recv, p_send, p_recv,
):
    rows, heads, width = q_hbm.shape
    kv = k_cut.shape[1]
    group = heads // kv
    flat = rows * group
    pair = 2 if n_ctx % 2 == 0 else 1
    chips = n_ctx // pair
    blocks = pair
    factor = width ** (-0.5) * math.log2(math.e)
    tiles = rows // tile_rows
    slots = sk.shape[1]
    span = k_cut.shape[2]
    tall = v_turn.shape[2]
    columns = scores_a.shape[1]
    me = lax.axis_index("ctx")
    chip, core = me // pair, me % pair

    def device(chip_at, core_at):
        return {"ctx": chip_at * pair + core_at}

    def remote(src, dst, send, recv, target):
        return pltpu.make_async_remote_copy(
            src_ref=src, dst_ref=dst, send_sem=send, recv_sem=recv,
            device_id=target, device_id_type=pl.DeviceIdType.MESH,
        )

    q_copy = pltpu.make_async_copy(q_hbm, q_raw.at[0], q_sem)
    q_copy.start()
    kv_copies = [
        pltpu.make_async_copy(pk_hbm, k_raw, kv_sem.at[0]),
        pltpu.make_async_copy(pv_hbm, v_raw, kv_sem.at[1]),
    ]
    for copy in kv_copies:
        copy.start()

    def suffix_copies(tile):
        at = pl.ds(tile * tile_rows, tile_rows)
        return (
            pltpu.make_async_copy(sk_hbm.at[at], sk.at[at], suf_sem.at[tile, 0]),
            pltpu.make_async_copy(sv_hbm.at[at], sv.at[at], suf_sem.at[tile, 1]),
        )

    partners = [device(lax.rem(chip + t, chips), core) for t in range(1, chips)]
    backs = [device(lax.rem(chip - t + chips, chips), core) for t in range(1, chips)]
    twin = device(chip, pair - 1 - core)
    greeted = partners + ([twin] if pair == 2 else [])
    barrier = pltpu.get_barrier_semaphore() if greeted else None
    for target in greeted:
        pl.semaphore_signal(
            barrier, inc=1, device_id=target, device_id_type=pl.DeviceIdType.MESH
        )

    q_sends = [
        remote(q_hbm, q_raw.at[t + 1], q_send.at[t], q_recv.at[t], partners[t])
        for t in range(chips - 1)
    ]

    def start_tile(tile, carry):
        for copy in suffix_copies(tile):
            copy.start()
        return carry

    lax.fori_loop(0, tiles, start_tile, 0)

    def split_queries(slot):
        wide_q = q_raw[slot].astype(F32).reshape(rows, kv, group, width)
        for k in range(kv):
            qk[k, slot * flat : (slot + 1) * flat] = wide_q[:, k].reshape(flat, width).astype(BF16)

    piece = wide.shape[1]
    cut = piece // kv

    def rows_of(k):
        return pl.ds(k, cut, stride=kv) if kv > 1 else pl.ds(0, piece)

    def split_keys():
        def step(i, carry):
            wide[0] = k_raw[pl.ds(pl.multiple_of(i * piece, piece), piece), :].astype(F32)
            to = pl.ds(pl.multiple_of(i * cut, cut), cut)
            for k in range(kv):
                k_cut[0, k, to, :] = wide[0, rows_of(k), :].astype(BF16)
            return carry

        lax.fori_loop(0, span * kv // piece, step, 0)

    def turn_values():
        ones = (lax.broadcasted_iota(jnp.int32, (tall - width, span), 0) == 0).astype(F32)
        for k in range(kv):
            v_turn[0, k, width:tall, :] = ones.astype(BF16)
        for i in range(span * kv // piece):
            wide[1] = v_raw[i * piece : (i + 1) * piece, :].astype(F32)
            for k in range(kv):
                turned = jnp.transpose(wide[1, rows_of(k), :])
                v_turn[0, k, 0:width, i * cut : (i + 1) * cut] = turned.astype(BF16)

    def kv_sends(k):
        if pair == 1:
            return []
        return [
            remote(k_cut.at[0, k], k_cut.at[1, k], kv_send.at[k, 0], kv_recv.at[k, 0], twin),
            remote(v_turn.at[0, k], v_turn.at[1, k], kv_send.at[k, 1], kv_recv.at[k, 1], twin),
        ]

    def merge(one, two):
        top = jnp.maximum(one[0], two[0])
        a, b = jnp.exp2(one[0] - top), jnp.exp2(two[0] - top)
        return top, one[1] * a + two[1] * b, one[2] * a + two[2] * b

    buffers = ((scores_a, weights_a, top_a), (scores_b, weights_b, top_b))
    height = math.gcd(span, 256)

    def unit_scores(unit, at):
        block, k, tile = unit
        scores, _, tops = buffers[at]
        ask = qk[k, tile * columns : (tile + 1) * columns]
        top = None
        for j in range(span // height):
            part_of = slice(j * height, (j + 1) * height)
            x = dot_t(k_cut[block, k, part_of], ask)
            scores[part_of] = x
            x = jnp.max(x.reshape(height // 8, 8, columns), axis=0)
            top = x if top is None else jnp.maximum(top, x)
        tops[...] = jnp.broadcast_to(jnp.max(top, axis=0, keepdims=True), (8, columns))

    def unit_sums(unit, at):
        block, k, tile = unit
        scores, weights, tops = buffers[at]
        for j in range(span // height):
            part_of = slice(j * height, (j + 1) * height)
            x = scores[part_of].reshape(height // 8, 8, columns)
            x = jnp.exp2((x - tops[...][None]) * factor)
            weights[part_of] = x.reshape(height, columns).astype(BF16)
        out = jnp.dot(v_turn[block, k], weights[...], preferred_element_type=F32)
        top = tops[...] * factor
        to = slice(tile * columns, (tile + 1) * columns)
        if block > 0:
            old = top_all[k, :, to]
            new = jnp.maximum(old, top)
            a, b = jnp.exp2(old - new), jnp.exp2(top - new)
            out = acc_all[k, :, to] * a[0:1] + out * b[0:1]
            top = new
        if block < blocks - 1:
            acc_all[k, :, to] = out
            top_all[k, :, to] = top
            return
        first = lax.broadcasted_iota(jnp.int32, (8, LANES), 0) == 0
        for c in range(columns // LANES):
            at_c = tile * columns + c * LANES
            here = slice(c * LANES, (c + 1) * LANES)
            slot, within = at_c // flat, at_c % flat
            if slot == 0:
                acc_all[k, :, at_c : at_c + LANES] = out[:, here]
                top_all[k, :, at_c : at_c + LANES] = top[:, here]
            else:
                into = slice(within, within + LANES)
                part[slot - 1, k, 0:width, into] = out[0:width, here]
                part[slot - 1, k, width : width + 8, into] = jnp.where(
                    first, out[width : width + 8, here], top[:, here]
                )

    def partial_copy(t, k):
        return remote(part.at[t, k], got.at[t, k], p_send.at[t, k], p_recv.at[t, k], backs[t])

    def run_units(steps):
        counts = {unit_scores: 0, suffix_scores: 0}
        ready_steps = []
        for before, first, second, unit, after in steps:
            ready_steps.append((before, first, second, unit, counts[first] % 2, after))
            counts[first] += 1
        for i, (before, first, second, unit, at, after) in enumerate(ready_steps):
            if i == 0:
                before()
                first(unit, at)
            if i + 1 < len(ready_steps):
                before_next, first_next, _, unit_next, at_next, _ = ready_steps[i + 1]
                before_next()
                first_next(unit_next, at_next)
            second(unit, at)
            after()

    def nop():
        pass

    asks, nears, fars = (ask_a, ask_b), (near_a, near_b), (far_a, far_b)
    half = slots // 2
    lane = lax.broadcasted_iota(jnp.int32, (8, LANES), 1)
    sublane = lax.broadcasted_iota(jnp.int32, (8, LANES), 0)
    same_head = sublane % kv == lane % heads // group
    diagonal = lax.broadcasted_iota(jnp.int32, (LANES, LANES), 0) == lax.broadcasted_iota(
        jnp.int32, (LANES, LANES), 1
    )

    def upright(row):
        wide_row = jnp.broadcast_to(row, (LANES, LANES))
        return jnp.sum(jnp.where(diagonal, wide_row, 0.0), axis=1, keepdims=True)

    def turn_queries():
        turned = jnp.transpose(q_raw[0].astype(F32).reshape(rows * heads, width)).astype(BF16)
        for tile in range(tiles):
            q_turn[tile] = turned[:, tile * LANES : (tile + 1) * LANES]

    def suffix_scores(tile, at):
        for copy in suffix_copies(tile):
            copy.wait()
        r0 = tile * tile_rows
        ask, (near, far) = asks[at], (nears[at], fars[at])
        turned = q_turn[tile]
        row_of = lax.broadcasted_iota(jnp.int32, (width, LANES), 1) // heads
        limit = jnp.zeros((8, LANES), jnp.int32)
        for r in range(tile_rows):
            mine = jnp.where(row_of == r, turned, jnp.zeros_like(turned))
            ask[2 * r * width : (2 * r + 1) * width, 0:LANES] = mine
            ask[(2 * r + 1) * width : (2 * r + 2) * width, LANES : 2 * LANES] = mine
            limit = jnp.where(lane // heads == r, len_ref[r0 + r] * kv, limit)
        limit = jnp.where(same_head, limit, -1)
        keys = jnp.concatenate(
            [sk[r0 + r, i * half : (i + 1) * half] for r in range(tile_rows) for i in range(2)], axis=1
        )
        both = jnp.dot(keys, ask[...], preferred_element_type=F32).reshape(half // 8, 8, 2 * LANES)
        slot = sublane[None] + 8 * lax.broadcasted_iota(jnp.int32, (half // 8, 8, LANES), 0)
        top = None
        for i in range(2):
            x = jnp.where(
                slot < (limit - i * half)[None], both[:, :, i * LANES : (i + 1) * LANES], MASKED
            )
            near[i] = x
            x = jnp.max(x, axis=0)
            top = x if top is None else jnp.maximum(top, x)
        far[...] = jnp.broadcast_to(jnp.max(top, axis=0, keepdims=True), (8, LANES))

    def suffix_sums(tile, at):
        r0 = tile * tile_rows
        near, far = nears[at], fars[at]
        total, parts = None, []
        for i in range(2):
            x = jnp.exp2((near[i] - far[...][None]) * factor).reshape(half, LANES).astype(BF16)
            y = jnp.sum(x.astype(F32).reshape(half // 8, 8, LANES), axis=0)
            total = y if total is None else total + y
            parts.append(jnp.transpose(x))
        weights = jnp.concatenate(parts, axis=1)
        total = jnp.sum(total, axis=0, keepdims=True)
        top = jnp.broadcast_to(upright(far[0:1] * factor), (LANES, width))
        total = jnp.broadcast_to(upright(total), (LANES, width))
        for r in range(tile_rows):
            acc = jnp.dot(weights[r * heads : (r + 1) * heads], sv[r0 + r], preferred_element_type=F32)
            to = slice((r0 + r) * group, (r0 + r + 1) * group)
            for k in range(kv):
                here = slice(r * heads + k * group, r * heads + (k + 1) * group)
                suf_acc[k, to, :] = acc[k * group : (k + 1) * group]
                suf_top[k, to, :] = top[here]
                suf_sum[k, to, :] = total[here]

    all_tiles = chips * flat // columns
    near = flat // columns

    q_copy.wait()
    split_queries(0)
    kv_copies[0].wait()
    split_keys()
    if greeted:
        pl.semaphore_wait(barrier, len(greeted))
    for copy in q_sends:
        copy.start()
    kv_copies[1].wait()
    turn_values()
    for k in range(kv):
        for copy in kv_sends(k):
            copy.start()
    turn_queries()
    for ask in asks:
        ask[...] = jnp.zeros(ask.shape, BF16)

    near_tiles = flat // columns
    all_tiles = chips * flat // columns
    waited = set()

    def ready(block, k, tile):
        def go():
            last = ((tile + 1) * columns - 1) // flat
            for t in range(last):
                if ("q", t) not in waited:
                    waited.add(("q", t))
                    q_sends[t].wait_recv()
                    split_queries(t + 1)
            if block > 0 and ("kv", k) not in waited:
                waited.add(("kv", k))
                for copy in kv_sends(k):
                    copy.wait_recv()

        return go

    def finish(block, k, tile):
        def go():
            if block == blocks - 1:
                for t in range(chips - 1):
                    end = (t + 2) * flat
                    if tile * columns < end <= (tile + 1) * columns:
                        partial_copy(t, k).start()

        return go

    def documents(order):
        return [
            (ready(*unit), unit_scores, unit_sums, unit, finish(*unit)) for unit in order
        ]

    def suffixes(tiles_of):
        return [(nop, suffix_scores, suffix_sums, tile, nop) for tile in tiles_of]

    cut_at = tiles // 2
    run_units(
        documents([(0, k, tile) for tile in range(near_tiles) for k in range(kv)])
        + suffixes(range(cut_at))
        + documents(
            [
                (block, k, tile)
                for k in range(kv)
                for tile in range(near_tiles, all_tiles)
                for block in range(blocks)
            ]
        )
        + documents(
            [(block, k, tile) for k in range(kv) for tile in range(near_tiles) for block in range(1, blocks)]
        )
        + suffixes(range(cut_at, tiles))
    )

    for k in range(kv):
        for t in range(chips - 1):
            partial_copy(t, k).wait_recv()
    per = LANES // group
    for c in range(flat // LANES):
        at = slice(c * LANES, (c + 1) * LANES)
        done = []
        for k in range(kv):
            terms = (
                top_all[k, 0:1, at],
                acc_all[k, 0:width, at],
                acc_all[k, width : width + 1, at],
            )
            for t in range(chips - 1):
                terms = merge(
                    terms,
                    (
                        got[t, k, width + 1 : width + 2, at],
                        got[t, k, 0:width, at],
                        got[t, k, width : width + 1, at],
                    ),
                )
            terms = merge(
                (upright(terms[0]), jnp.transpose(terms[1]), upright(terms[2])),
                (suf_top[k, at, :], suf_acc[k, at, :], suf_sum[k, at, :]),
            )
            done.append((terms[1] / terms[2]).reshape(per, 1, group, width))
        joined = jnp.concatenate(done, axis=1).reshape(per, heads, width)
        out_ref[c * per : (c + 1) * per] = joined.astype(BF16)
    for copy in q_sends:
        copy.wait_send()
    for k in range(kv):
        for copy in kv_sends(k):
            copy.wait_send()
        for t in range(chips - 1):
            partial_copy(t, k).wait_send()


def shards(n_ctx, queries, prefix_keys, prefix_values, suffix_keys, suffix_values, lengths):
    rows, heads, width = queries.shape
    positions, kv, _ = prefix_keys.shape
    slots = suffix_keys.shape[1] * kv
    flat = rows * (heads // kv)
    pair = 2 if n_ctx % 2 == 0 else 1
    others = max(1, n_ctx // pair - 1)
    tile_rows = LANES // heads
    tiles = rows // tile_rows
    columns = math.gcd(n_ctx // pair * flat, 256)
    tall = width + 16
    piece = math.gcd(positions * kv, 1024)
    anywhere = pl.BlockSpec(memory_space=pl.ANY)
    vmem = pltpu.VMEM
    dma = pltpu.SemaphoreType.DMA
    call = pl.pallas_call(
        functools.partial(kernel, n_ctx, tile_rows),
        out_shape=jax.ShapeDtypeStruct((rows, heads, width), BF16),
        in_specs=[pl.BlockSpec(memory_space=pltpu.SMEM)] + [anywhere] * 5,
        out_specs=pl.BlockSpec(memory_space=vmem),
        scratch_shapes=[
            vmem((1 + others, rows, heads, width), BF16),
            vmem((kv, n_ctx // pair * flat, width), BF16),
            vmem((positions * kv, width), BF16),
            vmem((positions * kv, width), BF16),
            vmem((pair, kv, positions, width), BF16),
            vmem((pair, kv, tall, positions), BF16),
            vmem((2, piece, width), F32),
            vmem((rows, slots, width), BF16),
            vmem((rows, slots, width), BF16),
            vmem((positions, columns), F32),
            vmem((positions, columns), F32),
            vmem((positions, columns), BF16),
            vmem((positions, columns), BF16),
            vmem((8, columns), F32),
            vmem((8, columns), F32),
            vmem((2 * tile_rows * width, 2 * LANES), BF16),
            vmem((2 * tile_rows * width, 2 * LANES), BF16),
            vmem((2, slots // 16, 8, LANES), F32),
            vmem((2, slots // 16, 8, LANES), F32),
            vmem((8, LANES), F32),
            vmem((8, LANES), F32),
            vmem((kv, tall, n_ctx // pair * flat), F32),
            vmem((kv, 8, n_ctx // pair * flat), F32),
            vmem((others, kv, width + 8, flat), F32),
            vmem((others, kv, width + 8, flat), F32),
        ]
        + [vmem((tiles, width, LANES), BF16)]
        + [vmem((kv, flat, width), F32)] * 3
        + [
            dma,
            dma((2,)),
            dma((tiles, 2)),
            dma((others,)),
            dma((others,)),
            dma((kv, 2)),
            dma((kv, 2)),
            dma((others, kv)),
            dma((others, kv)),
        ],
        compiler_params=pltpu.CompilerParams(
            collective_id=0, has_side_effects=True, vmem_limit_bytes=62 * 1024 * 1024
        ),
    )
    return call(
        lengths,
        queries,
        prefix_keys.reshape(positions * kv, width),
        prefix_values.reshape(positions * kv, width),
        suffix_keys.reshape(rows, slots, width),
        suffix_values.reshape(rows, slots, width),
    )


def solution(mesh):
    placed = (
        P(("groups", "ctx"), "head", None),
        P(("groups", "ctx"), "head", None),
        P(("groups", "ctx"), "head", None),
        P(("groups", "ctx"), None, "head", None),
        P(("groups", "ctx"), None, "head", None),
        P(("groups", "ctx")),
    )
    return jax.shard_map(
        functools.partial(shards, mesh.shape["ctx"]),
        mesh=mesh,
        in_specs=placed,
        out_specs=P(("groups", "ctx"), "head", None),
        check_vma=False,
    )
```

```python
import functools
import math

import jax
import jax.numpy as jnp
from jax import lax
from jax.experimental import pallas as pl
from jax.experimental.pallas import tpu as pltpu
from jax.sharding import PartitionSpec as P

F32 = jnp.float32
BF16 = jnp.bfloat16
MASKED = -1e30
LANES = 128
CODES = 32767.0


def dot_t(a, b):
    return lax.dot_general(a, b, (((1,), (1,)), ((), ())), preferred_element_type=F32)


def kernel(
    n_ctx, tile_rows,
    len_ref, q_hbm, pk_hbm, pv_hbm, sk_hbm, sv_hbm, out_ref,
    q_raw, qk, k_raw, v_raw, k_cut, v_turn, wide, sk, sv,
    scores_a, scores_b, weights_a, weights_b, top_a, top_b,
    ask_a, ask_b, near_a, near_b, far_a, far_b, acc_all, top_all, part, got, part_stat, got_stat, q_turn, suf_acc, suf_top, suf_sum,
    q_sem, kv_sem, suf_sem, q_send, q_recv, kv_send, kv_recv, p_send, p_recv,
):
    rows, heads, width = q_hbm.shape
    kv = k_cut.shape[1]
    group = heads // kv
    flat = rows * group
    pair = 2 if n_ctx % 2 == 0 else 1
    chips = n_ctx // pair
    blocks = pair
    factor = width ** (-0.5) * math.log2(math.e)
    tiles = rows // tile_rows
    slots = sk.shape[1]
    span = k_cut.shape[2]
    tall = v_turn.shape[2]
    columns = scores_a.shape[1]
    me = lax.axis_index("ctx")
    chip, core = me // pair, me % pair

    def device(chip_at, core_at):
        return {"ctx": chip_at * pair + core_at}

    def remote(src, dst, send, recv, target):
        return pltpu.make_async_remote_copy(
            src_ref=src, dst_ref=dst, send_sem=send, recv_sem=recv,
            device_id=target, device_id_type=pl.DeviceIdType.MESH,
        )

    q_copy = pltpu.make_async_copy(q_hbm, q_raw.at[0], q_sem)
    q_copy.start()
    kv_copies = [
        pltpu.make_async_copy(pk_hbm, k_raw, kv_sem.at[0]),
        pltpu.make_async_copy(pv_hbm, v_raw, kv_sem.at[1]),
    ]
    for copy in kv_copies:
        copy.start()

    def suffix_copies(tile):
        at = pl.ds(tile * tile_rows, tile_rows)
        return (
            pltpu.make_async_copy(sk_hbm.at[at], sk.at[at], suf_sem.at[tile, 0]),
            pltpu.make_async_copy(sv_hbm.at[at], sv.at[at], suf_sem.at[tile, 1]),
        )

    partners = [device(lax.rem(chip + t, chips), core) for t in range(1, chips)]
    backs = [device(lax.rem(chip - t + chips, chips), core) for t in range(1, chips)]
    twin = device(chip, pair - 1 - core)
    greeted = partners + ([twin] if pair == 2 else [])
    barrier = pltpu.get_barrier_semaphore() if greeted else None
    for target in greeted:
        pl.semaphore_signal(
            barrier, inc=1, device_id=target, device_id_type=pl.DeviceIdType.MESH
        )

    row_pieces = [(0, rows)]
    q_sends = [
        [
            remote(
                q_hbm.at[lo:hi], q_raw.at[t + 1, lo:hi], q_send.at[t, i], q_recv.at[t, i], partners[t]
            )
            for i, (lo, hi) in enumerate(row_pieces)
        ]
        for t in range(chips - 1)
    ]

    def start_tile(tile, carry):
        for copy in suffix_copies(tile):
            copy.start()
        return carry

    lax.fori_loop(0, tiles, start_tile, 0)

    def split_queries(slot, lo, hi):
        wide_q = q_raw[slot, lo:hi].astype(F32).reshape(hi - lo, kv, group, width)
        for k in range(kv):
            qk[k, slot * flat + lo * group : slot * flat + hi * group] = (
                wide_q[:, k].reshape((hi - lo) * group, width).astype(BF16)
            )

    piece = wide.shape[1]
    cut = piece // kv

    def rows_of(k):
        return pl.ds(k, cut, stride=kv) if kv > 1 else pl.ds(0, piece)

    def split_keys():
        def step(i, carry):
            wide[0] = k_raw[pl.ds(pl.multiple_of(i * piece, piece), piece), :].astype(F32)
            to = pl.ds(pl.multiple_of(i * cut, cut), cut)
            for k in range(kv):
                k_cut[0, k, to, :] = wide[0, rows_of(k), :].astype(BF16)
            return carry

        lax.fori_loop(0, span * kv // piece, step, 0)

    def turn_values():
        ones = (lax.broadcasted_iota(jnp.int32, (tall - width, span), 0) == 0).astype(F32)
        for k in range(kv):
            v_turn[0, k, width:tall, :] = ones.astype(BF16)
        for i in range(span * kv // piece):
            wide[1] = v_raw[i * piece : (i + 1) * piece, :].astype(F32)
            for k in range(kv):
                turned = jnp.transpose(wide[1, rows_of(k), :])
                v_turn[0, k, 0:width, i * cut : (i + 1) * cut] = turned.astype(BF16)

    def kv_sends(k):
        if pair == 1:
            return []
        return [
            remote(k_cut.at[0, k], k_cut.at[1, k], kv_send.at[k, 0], kv_recv.at[k, 0], twin),
            remote(v_turn.at[0, k], v_turn.at[1, k], kv_send.at[k, 1], kv_recv.at[k, 1], twin),
        ]

    def merge(one, two):
        top = jnp.maximum(one[0], two[0])
        a, b = jnp.exp2(one[0] - top), jnp.exp2(two[0] - top)
        return top, one[1] * a + two[1] * b, one[2] * a + two[2] * b

    buffers = ((scores_a, weights_a, top_a), (scores_b, weights_b, top_b))
    height = math.gcd(span, 256)

    def unit_scores(unit, at):
        block, k, tile = unit
        scores, _, tops = buffers[at]
        ask = qk[k, tile * columns : (tile + 1) * columns]
        top = None
        for j in range(span // height):
            part_of = slice(j * height, (j + 1) * height)
            x = dot_t(k_cut[block, k, part_of], ask)
            scores[part_of] = x
            x = jnp.max(x.reshape(height // 8, 8, columns), axis=0)
            top = x if top is None else jnp.maximum(top, x)
        tops[...] = jnp.broadcast_to(jnp.max(top, axis=0, keepdims=True), (8, columns))

    def unit_sums(unit, at):
        block, k, tile = unit
        scores, weights, tops = buffers[at]
        for j in range(span // height):
            part_of = slice(j * height, (j + 1) * height)
            x = scores[part_of].reshape(height // 8, 8, columns)
            x = jnp.exp2((x - tops[...][None]) * factor)
            weights[part_of] = x.reshape(height, columns).astype(BF16)
        out = jnp.dot(v_turn[block, k], weights[...], preferred_element_type=F32)
        top = tops[...] * factor
        to = slice(tile * columns, (tile + 1) * columns)
        if block > 0:
            old = top_all[k, :, to]
            new = jnp.maximum(old, top)
            a, b = jnp.exp2(old - new), jnp.exp2(top - new)
            out = acc_all[k, :, to] * a[0:1] + out * b[0:1]
            top = new
        if block < blocks - 1:
            acc_all[k, :, to] = out
            top_all[k, :, to] = top
            return
        row = lax.broadcasted_iota(jnp.int32, (8, LANES), 0)
        for c in range(columns // LANES):
            at_c = tile * columns + c * LANES
            here = slice(c * LANES, (c + 1) * LANES)
            slot, within = at_c // flat, at_c % flat
            if slot == 0:
                acc_all[k, :, at_c : at_c + LANES] = out[:, here]
                top_all[k, :, at_c : at_c + LANES] = top[:, here]
            else:
                into = slice(within, within + LANES)
                x = out[0:width, here]
                most = jnp.max(jnp.max(jnp.abs(x).reshape(width // 8, 8, LANES), axis=0), axis=0, keepdims=True)
                most = jnp.maximum(most, 1e-33)
                code = jnp.round(x * (CODES / most)).astype(jnp.int32)
                part[slot - 1, k, :, into] = code.astype(jnp.int16)
                stat = jnp.where(row == 1, top[:, here], most * (1.0 / CODES))
                part_stat[slot - 1, k, :, into] = jnp.where(row == 0, out[width : width + 8, here], stat)

    def partial_copies(t, k, i):
        at = slice(row_pieces[i][0] * group, row_pieces[i][1] * group)
        return [
            remote(
                src.at[t, k, :, at], dst.at[t, k, :, at], p_send.at[t, k, i, j], p_recv.at[t, k, i, j], backs[t]
            )
            for j, (src, dst) in enumerate(((part, got), (part_stat, got_stat)))
        ]

    def run_units(steps):
        counts = {unit_scores: 0, suffix_scores: 0}
        ready_steps = []
        for before, first, second, unit, after in steps:
            ready_steps.append((before, first, second, unit, counts[first] % 2, after))
            counts[first] += 1
        for i, (before, first, second, unit, at, after) in enumerate(ready_steps):
            if i == 0:
                before()
                first(unit, at)
                settle()
            if i + 1 < len(ready_steps):
                before_next, first_next, _, unit_next, at_next, _ = ready_steps[i + 1]
                before_next()
                first_next(unit_next, at_next)
            second(unit, at)
            after()

    def nop():
        pass

    asks, nears, fars = (ask_a, ask_b), (near_a, near_b), (far_a, far_b)
    half = slots // 2
    lane = lax.broadcasted_iota(jnp.int32, (8, LANES), 1)
    sublane = lax.broadcasted_iota(jnp.int32, (8, LANES), 0)
    same_head = sublane % kv == lane % heads // group
    diagonal = lax.broadcasted_iota(jnp.int32, (LANES, LANES), 0) == lax.broadcasted_iota(
        jnp.int32, (LANES, LANES), 1
    )

    def upright(row):
        wide_row = jnp.broadcast_to(row, (LANES, LANES))
        return jnp.sum(jnp.where(diagonal, wide_row, 0.0), axis=1, keepdims=True)

    def turn_queries():
        turned = jnp.transpose(q_raw[0].astype(F32).reshape(rows * heads, width)).astype(BF16)
        for tile in range(tiles):
            q_turn[tile] = turned[:, tile * LANES : (tile + 1) * LANES]

    def suffix_scores(tile, at):
        r0 = tile * tile_rows
        ask, (near, far) = asks[at], (nears[at], fars[at])
        turned = q_turn[tile]
        row_of = lax.broadcasted_iota(jnp.int32, (width, LANES), 1) // heads
        limit = jnp.zeros((8, LANES), jnp.int32)
        for r in range(tile_rows):
            mine = jnp.where(row_of == r, turned, jnp.zeros_like(turned))
            ask[2 * r * width : (2 * r + 1) * width, 0:LANES] = mine
            ask[(2 * r + 1) * width : (2 * r + 2) * width, LANES : 2 * LANES] = mine
            limit = jnp.where(lane // heads == r, len_ref[r0 + r] * kv, limit)
        limit = jnp.where(same_head, limit, -1)
        keys = jnp.concatenate(
            [sk[r0 + r, i * half : (i + 1) * half] for r in range(tile_rows) for i in range(2)], axis=1
        )
        both = jnp.dot(keys, ask[...], preferred_element_type=F32).reshape(half // 8, 8, 2 * LANES)
        slot = sublane[None] + 8 * lax.broadcasted_iota(jnp.int32, (half // 8, 8, LANES), 0)
        top = None
        for i in range(2):
            x = jnp.where(
                slot < (limit - i * half)[None], both[:, :, i * LANES : (i + 1) * LANES], MASKED
            )
            near[i] = x
            x = jnp.max(x, axis=0)
            top = x if top is None else jnp.maximum(top, x)
        far[...] = jnp.broadcast_to(jnp.max(top, axis=0, keepdims=True), (8, LANES))

    def suffix_sums(tile, at):
        r0 = tile * tile_rows
        near, far = nears[at], fars[at]
        total, parts = None, []
        for i in range(2):
            x = jnp.exp2((near[i] - far[...][None]) * factor).reshape(half, LANES).astype(BF16)
            y = jnp.sum(x.astype(F32).reshape(half // 8, 8, LANES), axis=0)
            total = y if total is None else total + y
            parts.append(jnp.transpose(x))
        weights = jnp.concatenate(parts, axis=1)
        total = jnp.sum(total, axis=0, keepdims=True)
        top = jnp.broadcast_to(upright(far[0:1] * factor), (LANES, width))
        total = jnp.broadcast_to(upright(total), (LANES, width))
        for r in range(tile_rows):
            acc = jnp.dot(weights[r * heads : (r + 1) * heads], sv[r0 + r], preferred_element_type=F32)
            to = slice((r0 + r) * group, (r0 + r + 1) * group)
            for k in range(kv):
                here = slice(r * heads + k * group, r * heads + (k + 1) * group)
                suf_acc[k, to, :] = acc[k * group : (k + 1) * group]
                suf_top[k, to, :] = top[here]
                suf_sum[k, to, :] = total[here]

    all_tiles = chips * flat // columns
    near = flat // columns

    def send_queries():
        if greeted:
            pl.semaphore_wait(barrier, len(greeted))
        for i in range(len(row_pieces)):
            for t in range(chips - 1):
                q_sends[t][i].start()
        for k in range(kv):
            for copy in kv_sends(k)[:1]:
                copy.start()

    def settle():
        kv_copies[1].wait()
        turn_values()
        for k in range(kv):
            for copy in kv_sends(k)[1:]:
                copy.start()
        turn_queries()
        for ask in asks:
            ask[...] = jnp.zeros(ask.shape, BF16)

    q_copy.wait()
    split_queries(0, 0, rows)
    kv_copies[0].wait()
    split_keys()
    send_queries()

    near_tiles = flat // columns
    all_tiles = chips * flat // columns
    waited = set()

    def ready(block, k, tile):
        def go():
            for t in range(chips - 1):
                for i, (lo, hi) in enumerate(row_pieces):
                    begin = (t + 1) * flat + lo * group
                    if begin < (tile + 1) * columns and ("q", t, i) not in waited:
                        waited.add(("q", t, i))
                        q_sends[t][i].wait_recv()
                        split_queries(t + 1, lo, hi)
            if block > 0 and "kv" not in waited:
                waited.add("kv")
                for each in range(kv):
                    for copy in kv_sends(each):
                        copy.wait_recv()

        return go

    finished = set()

    def finish(block, k, tile):
        def go():
            if block < blocks - 1:
                return
            finished.update((k, at) for at in range(tile * columns, (tile + 1) * columns, LANES))
            for t in range(chips - 1):
                for i, (lo, hi) in enumerate(row_pieces):
                    begin, end = (t + 1) * flat + lo * group, (t + 1) * flat + hi * group
                    done = all((k, at) in finished for at in range(begin, end, LANES))
                    if done and ("p", t, k, i) not in waited:
                        waited.add(("p", t, k, i))
                        for copy in partial_copies(t, k, i):
                            copy.start()

        return go

    def documents(order):
        return [
            (ready(*unit), unit_scores, unit_sums, unit, finish(*unit)) for unit in order
        ]

    def arrived(tiles_of):
        def go():
            for tile in tiles_of:
                for copy in suffix_copies(tile):
                    copy.wait()

        return go

    def suffixes(tiles_of, together=False):
        steps = []
        for tile in tiles_of:
            need = ([tile] if not together else list(tiles_of) if tile == tiles_of[0] else [])
            steps.append((arrived(need), suffix_scores, suffix_sums, tile, nop))
        return steps

    own_first = documents([(0, k, tile) for tile in range(near_tiles) for k in range(kv)])
    own_rest = documents(
        [(block, k, tile) for block in range(1, blocks) for tile in range(near_tiles) for k in range(kv)]
    )
    others = documents(
        [
            (block, k, tile)
            for k in range(kv)
            for tile in range(near_tiles, all_tiles)
            for block in range(blocks)
        ]
    )
    early = tiles // 3
    run_units(
        own_first
        + suffixes(range(early))
        + own_rest
        + others
        + suffixes(range(early, tiles), True)
    )

    for k in range(kv):
        for t in range(chips - 1):
            for i in range(len(row_pieces)):
                for copy in partial_copies(t, k, i):
                    copy.wait_recv()
    per = LANES // group
    for c in range(flat // LANES):
        at = slice(c * LANES, (c + 1) * LANES)
        done = []
        for k in range(kv):
            terms = (
                top_all[k, 0:1, at],
                acc_all[k, 0:width, at],
                acc_all[k, width : width + 1, at],
            )
            for t in range(chips - 1):
                terms = merge(
                    terms,
                    (
                        got_stat[t, k, 1:2, at],
                        got[t, k, :, at].astype(jnp.int32).astype(F32) * got_stat[t, k, 2:3, at],
                        got_stat[t, k, 0:1, at],
                    ),
                )
            terms = merge(
                (upright(terms[0]), jnp.transpose(terms[1]), upright(terms[2])),
                (suf_top[k, at, :], suf_acc[k, at, :], suf_sum[k, at, :]),
            )
            done.append((terms[1] / terms[2]).reshape(per, 1, group, width))
        joined = jnp.concatenate(done, axis=1).reshape(per, heads, width)
        out_ref[c * per : (c + 1) * per] = joined.astype(BF16)
    for copies in q_sends:
        for copy in copies:
            copy.wait_send()
    for k in range(kv):
        for copy in kv_sends(k):
            copy.wait_send()
        for t in range(chips - 1):
            for i in range(len(row_pieces)):
                for copy in partial_copies(t, k, i):
                    copy.wait_send()


def shards(n_ctx, queries, prefix_keys, prefix_values, suffix_keys, suffix_values, lengths):
    rows, heads, width = queries.shape
    positions, kv, _ = prefix_keys.shape
    slots = suffix_keys.shape[1] * kv
    flat = rows * (heads // kv)
    pair = 2 if n_ctx % 2 == 0 else 1
    others = max(1, n_ctx // pair - 1)
    tile_rows = LANES // heads
    tiles = rows // tile_rows
    columns = math.gcd(n_ctx // pair * flat, 256)
    tall = width + 16
    piece = math.gcd(positions * kv, 1024)
    anywhere = pl.BlockSpec(memory_space=pl.ANY)
    vmem = pltpu.VMEM
    dma = pltpu.SemaphoreType.DMA
    call = pl.pallas_call(
        functools.partial(kernel, n_ctx, tile_rows),
        out_shape=jax.ShapeDtypeStruct((rows, heads, width), BF16),
        in_specs=[pl.BlockSpec(memory_space=pltpu.SMEM)] + [anywhere] * 5,
        out_specs=pl.BlockSpec(memory_space=vmem),
        scratch_shapes=[
            vmem((1 + others, rows, heads, width), BF16),
            vmem((kv, n_ctx // pair * flat, width), BF16),
            vmem((positions * kv, width), BF16),
            vmem((positions * kv, width), BF16),
            vmem((pair, kv, positions, width), BF16),
            vmem((pair, kv, tall, positions), BF16),
            vmem((2, piece, width), F32),
            vmem((rows, slots, width), BF16),
            vmem((rows, slots, width), BF16),
            vmem((positions, columns), F32),
            vmem((positions, columns), F32),
            vmem((positions, columns), BF16),
            vmem((positions, columns), BF16),
            vmem((8, columns), F32),
            vmem((8, columns), F32),
            vmem((2 * tile_rows * width, 2 * LANES), BF16),
            vmem((2 * tile_rows * width, 2 * LANES), BF16),
            vmem((2, slots // 16, 8, LANES), F32),
            vmem((2, slots // 16, 8, LANES), F32),
            vmem((8, LANES), F32),
            vmem((8, LANES), F32),
            vmem((kv, tall, n_ctx // pair * flat), F32),
            vmem((kv, 8, n_ctx // pair * flat), F32),
            vmem((others, kv, width, flat), jnp.int16),
            vmem((others, kv, width, flat), jnp.int16),
            vmem((others, kv, 8, flat), F32),
            vmem((others, kv, 8, flat), F32),
        ]
        + [vmem((tiles, width, LANES), BF16)]
        + [vmem((kv, flat, width), F32)] * 3
        + [
            dma,
            dma((2,)),
            dma((tiles, 2)),
            dma((others, 2)),
            dma((others, 2)),
            dma((kv, 2)),
            dma((kv, 2)),
            dma((others, kv, 2, 2)),
            dma((others, kv, 2, 2)),
        ],
        compiler_params=pltpu.CompilerParams(
            collective_id=0, has_side_effects=True, vmem_limit_bytes=62 * 1024 * 1024
        ),
    )
    return call(
        lengths,
        queries,
        prefix_keys.reshape(positions * kv, width),
        prefix_values.reshape(positions * kv, width),
        suffix_keys.reshape(rows, slots, width),
        suffix_values.reshape(rows, slots, width),
    )


def solution(mesh):
    placed = (
        P(("groups", "ctx"), "head", None),
        P(("groups", "ctx"), "head", None),
        P(("groups", "ctx"), "head", None),
        P(("groups", "ctx"), None, "head", None),
        P(("groups", "ctx"), None, "head", None),
        P(("groups", "ctx")),
    )
    return jax.shard_map(
        functools.partial(shards, mesh.shape["ctx"]),
        mesh=mesh,
        in_specs=placed,
        out_specs=P(("groups", "ctx"), "head", None),
        check_vma=False,
    )
```

```python
import functools
import math

import jax
import jax.numpy as jnp
from jax import lax
from jax.experimental import pallas as pl
from jax.experimental.pallas import tpu as pltpu
from jax.sharding import PartitionSpec as P

F32 = jnp.float32
BF16 = jnp.bfloat16
MASKED = -1e30
LANES = 128
CODES = 32767.0


def dot_t(a, b):
    return lax.dot_general(a, b, (((1,), (1,)), ((), ())), preferred_element_type=F32)


def kernel(
    n_ctx, tile_rows,
    len_hbm, q_hbm, pk_hbm, pv_hbm, sk_hbm, sv_hbm, out_ref,
    len_ref,
    q_raw, qk, k_raw, v_raw, k_cut, v_turn, wide, sk, sv,
    scores_a, scores_b, weights_a, weights_b, top_a, top_b,
    ask_a, ask_b, near_a, near_b, far_a, far_b, acc_all, top_all, part, got, part_stat, got_stat, q_turn, suf_acc, suf_top, suf_sum,
    len_sem, q_sem, kv_sem, suf_sem, q_send, q_recv, kv_send, kv_recv, p_send, p_recv,
):
    rows, heads, width = q_hbm.shape
    kv = k_cut.shape[1]
    group = heads // kv
    flat = rows * group
    pair = 2 if n_ctx % 2 == 0 else 1
    chips = n_ctx // pair
    blocks = pair
    factor = width ** (-0.5) * math.log2(math.e)
    tiles = rows // tile_rows
    slots = sk.shape[1]
    span = k_cut.shape[2]
    tall = v_turn.shape[2]
    columns = scores_a.shape[1]
    me = lax.axis_index("ctx")
    chip, core = me // pair, me % pair

    def device(chip_at, core_at):
        return {"ctx": chip_at * pair + core_at}

    def remote(src, dst, send, recv, target):
        return pltpu.make_async_remote_copy(
            src_ref=src, dst_ref=dst, send_sem=send, recv_sem=recv,
            device_id=target, device_id_type=pl.DeviceIdType.MESH,
        )

    q_copy = pltpu.make_async_copy(q_hbm, q_raw.at[0], q_sem)
    q_copy.start()
    kv_copies = [
        pltpu.make_async_copy(pk_hbm, k_raw, kv_sem.at[0]),
        pltpu.make_async_copy(pv_hbm, v_raw, kv_sem.at[1]),
    ]
    for copy in kv_copies:
        copy.start()
    len_copy = pltpu.make_async_copy(len_hbm, len_ref, len_sem)
    len_copy.start()

    def suffix_copies(tile):
        at = pl.ds(tile * tile_rows, tile_rows)
        return (
            pltpu.make_async_copy(sk_hbm.at[at], sk.at[at], suf_sem.at[tile, 0]),
            pltpu.make_async_copy(sv_hbm.at[at], sv.at[at], suf_sem.at[tile, 1]),
        )

    partners = [device(lax.rem(chip + t, chips), core) for t in range(1, chips)]
    backs = [device(lax.rem(chip - t + chips, chips), core) for t in range(1, chips)]
    twin = device(chip, pair - 1 - core)
    greeted = partners + ([twin] if pair == 2 else [])
    barrier = pltpu.get_barrier_semaphore() if greeted else None
    for target in greeted:
        pl.semaphore_signal(
            barrier, inc=1, device_id=target, device_id_type=pl.DeviceIdType.MESH
        )

    row_pieces = [(0, rows)]
    q_sends = [
        [
            remote(
                q_hbm.at[lo:hi], q_raw.at[t + 1, lo:hi], q_send.at[t, i], q_recv.at[t, i], partners[t]
            )
            for i, (lo, hi) in enumerate(row_pieces)
        ]
        for t in range(chips - 1)
    ]

    def start_tile(tile, carry):
        for copy in suffix_copies(tile):
            copy.start()
        return carry

    lax.fori_loop(0, tiles, start_tile, 0)

    def split_queries(slot, lo, hi):
        wide_q = q_raw[slot, lo:hi].astype(F32).reshape(hi - lo, kv, group, width)
        for k in range(kv):
            qk[k, slot * flat + lo * group : slot * flat + hi * group] = (
                wide_q[:, k].reshape((hi - lo) * group, width).astype(BF16)
            )

    piece = wide.shape[1]
    cut = piece // kv

    def rows_of(k):
        return pl.ds(k, cut, stride=kv) if kv > 1 else pl.ds(0, piece)

    def split_keys():
        def step(i, carry):
            wide[0] = k_raw[pl.ds(pl.multiple_of(i * piece, piece), piece), :].astype(F32)
            to = pl.ds(pl.multiple_of(i * cut, cut), cut)
            for k in range(kv):
                k_cut[0, k, to, :] = wide[0, rows_of(k), :].astype(BF16)
            return carry

        lax.fori_loop(0, span * kv // piece, step, 0)

    def turn_values():
        ones = (lax.broadcasted_iota(jnp.int32, (tall - width, span), 0) == 0).astype(F32)
        for k in range(kv):
            v_turn[0, k, width:tall, :] = ones.astype(BF16)
        for i in range(span * kv // piece):
            wide[1] = v_raw[i * piece : (i + 1) * piece, :].astype(F32)
            for k in range(kv):
                turned = jnp.transpose(wide[1, rows_of(k), :])
                v_turn[0, k, 0:width, i * cut : (i + 1) * cut] = turned.astype(BF16)

    def kv_sends(k):
        if pair == 1:
            return []
        return [
            remote(k_cut.at[0, k], k_cut.at[1, k], kv_send.at[k, 0], kv_recv.at[k, 0], twin),
            remote(v_turn.at[0, k], v_turn.at[1, k], kv_send.at[k, 1], kv_recv.at[k, 1], twin),
        ]

    def merge(one, two):
        top = jnp.maximum(one[0], two[0])
        a, b = jnp.exp2(one[0] - top), jnp.exp2(two[0] - top)
        return top, one[1] * a + two[1] * b, one[2] * a + two[2] * b

    buffers = ((scores_a, weights_a, top_a), (scores_b, weights_b, top_b))
    height = math.gcd(span, 256)

    def unit_scores(unit, at):
        block, k, tile = unit
        scores, _, tops = buffers[at]
        ask = qk[k, tile * columns : (tile + 1) * columns]
        top = None
        for j in range(span // height):
            part_of = slice(j * height, (j + 1) * height)
            x = dot_t(k_cut[block, k, part_of], ask)
            scores[part_of] = x
            x = jnp.max(x.reshape(height // 8, 8, columns), axis=0)
            top = x if top is None else jnp.maximum(top, x)
        tops[...] = jnp.broadcast_to(jnp.max(top, axis=0, keepdims=True), (8, columns))

    def unit_sums(unit, at):
        block, k, tile = unit
        scores, weights, tops = buffers[at]
        for j in range(span // height):
            part_of = slice(j * height, (j + 1) * height)
            x = scores[part_of].reshape(height // 8, 8, columns)
            x = jnp.exp2((x - tops[...][None]) * factor)
            weights[part_of] = x.reshape(height, columns).astype(BF16)
        out = jnp.dot(v_turn[block, k], weights[...], preferred_element_type=F32)
        top = tops[...] * factor
        to = slice(tile * columns, (tile + 1) * columns)
        if block > 0:
            old = top_all[k, :, to]
            new = jnp.maximum(old, top)
            a, b = jnp.exp2(old - new), jnp.exp2(top - new)
            out = acc_all[k, :, to] * a[0:1] + out * b[0:1]
            top = new
        if block < blocks - 1:
            acc_all[k, :, to] = out
            top_all[k, :, to] = top
            return
        row = lax.broadcasted_iota(jnp.int32, (8, LANES), 0)
        for c in range(columns // LANES):
            at_c = tile * columns + c * LANES
            here = slice(c * LANES, (c + 1) * LANES)
            slot, within = at_c // flat, at_c % flat
            if slot == 0:
                acc_all[k, :, at_c : at_c + LANES] = out[:, here]
                top_all[k, :, at_c : at_c + LANES] = top[:, here]
            else:
                into = slice(within, within + LANES)
                x = out[0:width, here]
                most = jnp.max(jnp.max(jnp.abs(x).reshape(width // 8, 8, LANES), axis=0), axis=0, keepdims=True)
                most = jnp.maximum(most, 1e-33)
                code = jnp.round(x * (CODES / most)).astype(jnp.int32)
                part[slot - 1, k, :, into] = code.astype(jnp.int16)
                stat = jnp.where(row == 1, top[:, here], most * (1.0 / CODES))
                part_stat[slot - 1, k, :, into] = jnp.where(row == 0, out[width : width + 8, here], stat)

    def partial_copies(t, k, i):
        at = slice(row_pieces[i][0] * group, row_pieces[i][1] * group)
        return [
            remote(
                src.at[t, k, :, at], dst.at[t, k, :, at], p_send.at[t, k, i, j], p_recv.at[t, k, i, j], backs[t]
            )
            for j, (src, dst) in enumerate(((part, got), (part_stat, got_stat)))
        ]

    split_at = (tiles - 1) * tile_rows * group // LANES

    def finals(lo, hi):
        per = LANES // group
        for c in range(lo, hi):
            at = slice(c * LANES, (c + 1) * LANES)
            done = []
            for k in range(kv):
                terms = (
                    top_all[k, 0:1, at],
                    acc_all[k, 0:width, at],
                    acc_all[k, width : width + 1, at],
                )
                for t in range(chips - 1):
                    terms = merge(
                        terms,
                        (
                            got_stat[t, k, 1:2, at],
                            got[t, k, :, at].astype(jnp.int32).astype(F32) * got_stat[t, k, 2:3, at],
                            got_stat[t, k, 0:1, at],
                        ),
                    )
                terms = merge(
                    (upright(terms[0]), jnp.transpose(terms[1]), upright(terms[2])),
                    (suf_top[k, at, :], suf_acc[k, at, :], suf_sum[k, at, :]),
                )
                done.append((terms[1] / terms[2]).reshape(per, 1, group, width))
            joined = jnp.concatenate(done, axis=1).reshape(per, heads, width)
            out_ref[c * per : (c + 1) * per] = joined.astype(BF16)

    def collect():
        for k in range(kv):
            for t in range(chips - 1):
                for i in range(len(row_pieces)):
                    for copy in partial_copies(t, k, i):
                        copy.wait_recv()
        finals(0, split_at)

    def run_units(steps):
        counts = {unit_scores: 0, suffix_scores: 0}
        ready_steps = []
        for before, first, second, unit, after in steps:
            ready_steps.append((before, first, second, unit, counts[first] % 2, after))
            counts[first] += 1
        for i, (before, first, second, unit, at, after) in enumerate(ready_steps):
            if i == 0:
                before()
                first(unit, at)
                kv_copies[1].wait()
                len_copy.wait()
            if i + 1 < len(ready_steps):
                before_next, first_next, _, unit_next, at_next, _ = ready_steps[i + 1]
                before_next()
                first_next(unit_next, at_next)
            if i == 0:
                settle()
            if i + 1 == len(ready_steps):
                collect()
            second(unit, at)
            after()

    def nop():
        pass

    asks, nears, fars = (ask_a, ask_b), (near_a, near_b), (far_a, far_b)
    half = slots // 2
    lane = lax.broadcasted_iota(jnp.int32, (8, LANES), 1)
    sublane = lax.broadcasted_iota(jnp.int32, (8, LANES), 0)
    same_head = sublane % kv == lane % heads // group
    diagonal = lax.broadcasted_iota(jnp.int32, (LANES, LANES), 0) == lax.broadcasted_iota(
        jnp.int32, (LANES, LANES), 1
    )

    def upright(row):
        wide_row = jnp.broadcast_to(row, (LANES, LANES))
        return jnp.sum(jnp.where(diagonal, wide_row, 0.0), axis=1, keepdims=True)

    def turn_queries():
        turned = jnp.transpose(q_raw[0].astype(F32).reshape(rows * heads, width)).astype(BF16)
        for tile in range(tiles):
            q_turn[tile] = turned[:, tile * LANES : (tile + 1) * LANES]

    def suffix_scores(tile, at):
        r0 = tile * tile_rows
        ask, (near, far) = asks[at], (nears[at], fars[at])
        turned = q_turn[tile]
        row_of = lax.broadcasted_iota(jnp.int32, (width, LANES), 1) // heads
        limit = jnp.zeros((8, LANES), jnp.int32)
        for r in range(tile_rows):
            mine = jnp.where(row_of == r, turned, jnp.zeros_like(turned))
            ask[2 * r * width : (2 * r + 1) * width, 0:LANES] = mine
            ask[(2 * r + 1) * width : (2 * r + 2) * width, LANES : 2 * LANES] = mine
            limit = jnp.where(lane // heads == r, len_ref[r0 + r] * kv, limit)
        limit = jnp.where(same_head, limit, -1)
        keys = jnp.concatenate(
            [sk[r0 + r, i * half : (i + 1) * half] for r in range(tile_rows) for i in range(2)], axis=1
        )
        both = jnp.dot(keys, ask[...], preferred_element_type=F32).reshape(half // 8, 8, 2 * LANES)
        slot = sublane[None] + 8 * lax.broadcasted_iota(jnp.int32, (half // 8, 8, LANES), 0)
        top = None
        for i in range(2):
            x = jnp.where(
                slot < (limit - i * half)[None], both[:, :, i * LANES : (i + 1) * LANES], MASKED
            )
            near[i] = x
            x = jnp.max(x, axis=0)
            top = x if top is None else jnp.maximum(top, x)
        far[...] = jnp.broadcast_to(jnp.max(top, axis=0, keepdims=True), (8, LANES))

    def suffix_sums(tile, at):
        r0 = tile * tile_rows
        near, far = nears[at], fars[at]
        total, parts = None, []
        for i in range(2):
            x = jnp.exp2((near[i] - far[...][None]) * factor).reshape(half, LANES).astype(BF16)
            y = jnp.sum(x.astype(F32).reshape(half // 8, 8, LANES), axis=0)
            total = y if total is None else total + y
            parts.append(jnp.transpose(x))
        weights = jnp.concatenate(parts, axis=1)
        total = jnp.sum(total, axis=0, keepdims=True)
        top = jnp.broadcast_to(upright(far[0:1] * factor), (LANES, width))
        total = jnp.broadcast_to(upright(total), (LANES, width))
        for r in range(tile_rows):
            acc = jnp.dot(weights[r * heads : (r + 1) * heads], sv[r0 + r], preferred_element_type=F32)
            to = slice((r0 + r) * group, (r0 + r + 1) * group)
            for k in range(kv):
                here = slice(r * heads + k * group, r * heads + (k + 1) * group)
                suf_acc[k, to, :] = acc[k * group : (k + 1) * group]
                suf_top[k, to, :] = top[here]
                suf_sum[k, to, :] = total[here]

    all_tiles = chips * flat // columns
    near = flat // columns

    def send_queries():
        if greeted:
            pl.semaphore_wait(barrier, len(greeted))
        for i in range(len(row_pieces)):
            for t in range(chips - 1):
                q_sends[t][i].start()
        for k in range(kv):
            for copy in kv_sends(k)[:1]:
                copy.start()

    def settle():
        turn_values()
        for k in range(kv):
            for copy in kv_sends(k)[1:]:
                copy.start()
        turn_queries()
        for ask in asks:
            ask[...] = jnp.zeros(ask.shape, BF16)

    q_copy.wait()
    split_queries(0, 0, rows)
    kv_copies[0].wait()
    split_keys()
    send_queries()

    early = tiles // 3
    near_tiles = flat // columns
    all_tiles = chips * flat // columns
    waited = set()

    def ready(block, k, tile):
        def go():
            for t in range(chips - 1):
                for i, (lo, hi) in enumerate(row_pieces):
                    begin = (t + 1) * flat + lo * group
                    if begin < (tile + 1) * columns and ("q", t, i) not in waited:
                        waited.add(("q", t, i))
                        q_sends[t][i].wait_recv()
                        split_queries(t + 1, lo, hi)
            if block > 0 and "kv" not in waited:
                waited.add("kv")
                for each in range(kv):
                    for copy in kv_sends(each):
                        copy.wait_recv()

        return go

    finished = set()

    def finish(block, k, tile):
        def go():
            if block < blocks - 1:
                return
            finished.update((k, at) for at in range(tile * columns, (tile + 1) * columns, LANES))
            for t in range(chips - 1):
                for i, (lo, hi) in enumerate(row_pieces):
                    begin, end = (t + 1) * flat + lo * group, (t + 1) * flat + hi * group
                    done = all((k, at) in finished for at in range(begin, end, LANES))
                    if done and ("p", t, k, i) not in waited:
                        waited.add(("p", t, k, i))
                        for copy in partial_copies(t, k, i):
                            copy.start()
                        if t == chips - 2:
                            take_suffixes()

        return go

    def documents(order):
        return [
            (ready(*unit), unit_scores, unit_sums, unit, finish(*unit)) for unit in order
        ]

    def arrived(tiles_of):
        def go():
            for tile in tiles_of:
                for copy in suffix_copies(tile):
                    copy.wait()

        return go

    def take_suffixes():
        if "rest" not in waited:
            waited.add("rest")
            arrived(range(early, tiles))()

    def suffixes(tiles_of):
        return [
            (arrived([tile]) if tile < early else take_suffixes, suffix_scores, suffix_sums, tile, nop)
            for tile in tiles_of
        ]

    own_first = documents([(0, k, tile) for tile in range(near_tiles) for k in range(kv)])
    own_rest = documents(
        [(block, k, tile) for block in range(1, blocks) for tile in range(near_tiles) for k in range(kv)]
    )
    others = documents(
        [
            (block, k, tile)
            for k in range(kv)
            for tile in range(near_tiles, all_tiles)
            for block in range(blocks)
        ]
    )
    run_units(
        own_first
        + suffixes(range(early))
        + own_rest
        + others
        + suffixes(range(early, tiles))
    )

    finals(split_at, flat // LANES)
    for copies in q_sends:
        for copy in copies:
            copy.wait_send()
    for k in range(kv):
        for copy in kv_sends(k):
            copy.wait_send()
        for t in range(chips - 1):
            for i in range(len(row_pieces)):
                for copy in partial_copies(t, k, i):
                    copy.wait_send()


def shards(n_ctx, queries, prefix_keys, prefix_values, suffix_keys, suffix_values, lengths):
    rows, heads, width = queries.shape
    positions, kv, _ = prefix_keys.shape
    slots = suffix_keys.shape[1] * kv
    flat = rows * (heads // kv)
    pair = 2 if n_ctx % 2 == 0 else 1
    others = max(1, n_ctx // pair - 1)
    tile_rows = LANES // heads
    tiles = rows // tile_rows
    columns = math.gcd(n_ctx // pair * flat, 256)
    tall = width + 16
    piece = math.gcd(positions * kv, 1024)
    anywhere = pl.BlockSpec(memory_space=pl.ANY)
    vmem = pltpu.VMEM
    dma = pltpu.SemaphoreType.DMA
    call = pl.pallas_call(
        functools.partial(kernel, n_ctx, tile_rows),
        out_shape=jax.ShapeDtypeStruct((rows, heads, width), BF16),
        in_specs=[anywhere] * 6,
        out_specs=pl.BlockSpec(memory_space=vmem),
        scratch_shapes=[
            pltpu.SMEM((rows,), jnp.int32),
            vmem((1 + others, rows, heads, width), BF16),
            vmem((kv, n_ctx // pair * flat, width), BF16),
            vmem((positions * kv, width), BF16),
            vmem((positions * kv, width), BF16),
            vmem((pair, kv, positions, width), BF16),
            vmem((pair, kv, tall, positions), BF16),
            vmem((2, piece, width), F32),
            vmem((rows, slots, width), BF16),
            vmem((rows, slots, width), BF16),
            vmem((positions, columns), F32),
            vmem((positions, columns), F32),
            vmem((positions, columns), BF16),
            vmem((positions, columns), BF16),
            vmem((8, columns), F32),
            vmem((8, columns), F32),
            vmem((2 * tile_rows * width, 2 * LANES), BF16),
            vmem((2 * tile_rows * width, 2 * LANES), BF16),
            vmem((2, slots // 16, 8, LANES), F32),
            vmem((2, slots // 16, 8, LANES), F32),
            vmem((8, LANES), F32),
            vmem((8, LANES), F32),
            vmem((kv, tall, n_ctx // pair * flat), F32),
            vmem((kv, 8, n_ctx // pair * flat), F32),
            vmem((others, kv, width, flat), jnp.int16),
            vmem((others, kv, width, flat), jnp.int16),
            vmem((others, kv, 8, flat), F32),
            vmem((others, kv, 8, flat), F32),
        ]
        + [vmem((tiles, width, LANES), BF16)]
        + [vmem((kv, flat, width), F32)] * 3
        + [
            dma,
            dma,
            dma((2,)),
            dma((tiles, 2)),
            dma((others, 2)),
            dma((others, 2)),
            dma((kv, 2)),
            dma((kv, 2)),
            dma((others, kv, 2, 2)),
            dma((others, kv, 2, 2)),
        ],
        compiler_params=pltpu.CompilerParams(
            collective_id=0, has_side_effects=True, vmem_limit_bytes=52 * 1024 * 1024
        ),
    )
    operands = (
        lengths,
        queries,
        prefix_keys.reshape(positions * kv, width),
        prefix_values.reshape(positions * kv, width),
        suffix_keys.reshape(rows, slots, width),
        suffix_values.reshape(rows, slots, width),
    )
    return call(*(pltpu.with_memory_space_constraint(x, pltpu.HBM) for x in operands))


def solution(mesh):
    placed = (
        P(("groups", "ctx"), "head", None),
        P(("groups", "ctx"), "head", None),
        P(("groups", "ctx"), "head", None),
        P(("groups", "ctx"), None, "head", None),
        P(("groups", "ctx"), None, "head", None),
        P(("groups", "ctx")),
    )
    return jax.shard_map(
        functools.partial(shards, mesh.shape["ctx"]),
        mesh=mesh,
        in_specs=placed,
        out_specs=P(("groups", "ctx"), "head", None),
        check_vma=False,
    )
```

```python
import functools
import math

import jax
import jax.numpy as jnp
from jax import lax
from jax.experimental import pallas as pl
from jax.experimental.pallas import tpu as pltpu
from jax.sharding import PartitionSpec as P

F32 = jnp.float32
BF16 = jnp.bfloat16
MASKED = -1e30
LANES = 128
CODES = 32767.0


def dot_t(a, b):
    return lax.dot_general(a, b, (((1,), (1,)), ((), ())), preferred_element_type=F32)


def kernel(
    n_ctx, tile_rows,
    len_hbm, q_hbm, pk_hbm, pv_hbm, sk_hbm, sv_hbm, out_ref,
    len_ref,
    q_raw, q_far, qk, k_raw, v_raw, k_cut, v_turn, wide, sk, sv,
    scores_a, scores_b, weights_a, weights_b, top_a, top_b,
    ask_a, ask_b, near_a, near_b, far_a, far_b, acc_all, top_all, part, got, part_stat, got_stat, q_turn, suf_acc, suf_top, suf_sum,
    len_sem, q_sem, kv_sem, suf_sem, q_send, q_recv, kv_send, kv_recv, p_send, p_recv,
):
    rows, heads, width = q_hbm.shape
    kv = k_cut.shape[1]
    group = heads // kv
    flat = rows * group
    pair = 2 if n_ctx % 2 == 0 else 1
    chips = n_ctx // pair
    blocks = pair
    factor = width ** (-0.5) * math.log2(math.e)
    tiles = rows // tile_rows
    slots = sk.shape[1]
    span = k_cut.shape[2]
    tall = v_turn.shape[2]
    columns = scores_a.shape[1]
    me = lax.axis_index("ctx")
    chip, core = me // pair, me % pair

    def device(chip_at, core_at):
        return {"ctx": chip_at * pair + core_at}

    def remote(src, dst, send, recv, target):
        return pltpu.make_async_remote_copy(
            src_ref=src, dst_ref=dst, send_sem=send, recv_sem=recv,
            device_id=target, device_id_type=pl.DeviceIdType.MESH,
        )

    q_copy = pltpu.make_async_copy(q_hbm, q_raw, q_sem)
    q_copy.start()
    kv_copies = [
        pltpu.make_async_copy(pk_hbm, k_raw, kv_sem.at[0]),
        pltpu.make_async_copy(pv_hbm, v_raw, kv_sem.at[1]),
    ]
    for copy in kv_copies:
        copy.start()
    len_copy = pltpu.make_async_copy(len_hbm, len_ref, len_sem)
    len_copy.start()

    def suffix_copies(tile):
        at = pl.ds(tile * tile_rows, tile_rows)
        return (
            pltpu.make_async_copy(sk_hbm.at[at], sk.at[at], suf_sem.at[tile, 0]),
            pltpu.make_async_copy(sv_hbm.at[at], sv.at[at], suf_sem.at[tile, 1]),
        )

    partners = [device(lax.rem(chip + t, chips), core) for t in range(1, chips)]
    backs = [device(lax.rem(chip - t + chips, chips), core) for t in range(1, chips)]
    twin = device(chip, pair - 1 - core)
    greeted = partners + ([twin] if pair == 2 else [])
    barrier = pltpu.get_barrier_semaphore() if greeted else None
    for target in greeted:
        pl.semaphore_signal(
            barrier, inc=1, device_id=target, device_id_type=pl.DeviceIdType.MESH
        )

    row_pieces = [(0, rows)]
    q_sends = [
        [
            remote(
                q_hbm.at[:, k * group : (k + 1) * group], q_far.at[t, k],
                q_send.at[t, k], q_recv.at[t, k], partners[t],
            )
            for k in range(kv)
        ]
        for t in range(chips - 1)
    ]

    def start_tile(tile, carry):
        for copy in suffix_copies(tile):
            copy.start()
        return carry

    lax.fori_loop(0, tiles, start_tile, 0)

    def split_queries():
        wide_q = q_raw[...].astype(F32).reshape(rows, kv, group, width)
        for k in range(kv):
            qk[k, 0:flat] = wide_q[:, k].reshape(flat, width).astype(BF16)

    def join_queries(t, k):
        far_q = q_far[t, k].astype(F32).reshape(flat, width).astype(BF16)
        qk[k, (t + 1) * flat : (t + 2) * flat] = far_q

    piece = wide.shape[1]
    cut = piece // kv

    def rows_of(k):
        return pl.ds(k, cut, stride=kv) if kv > 1 else pl.ds(0, piece)

    def split_keys():
        def step(i, carry):
            wide[0] = k_raw[pl.ds(pl.multiple_of(i * piece, piece), piece), :].astype(F32)
            to = pl.ds(pl.multiple_of(i * cut, cut), cut)
            for k in range(kv):
                k_cut[0, k, to, :] = wide[0, rows_of(k), :].astype(BF16)
            return carry

        lax.fori_loop(0, span * kv // piece, step, 0)

    def turn_values():
        ones = (lax.broadcasted_iota(jnp.int32, (tall - width, span), 0) == 0).astype(F32)
        for k in range(kv):
            v_turn[0, k, width:tall, :] = ones.astype(BF16)
        for i in range(span * kv // piece):
            wide[1] = v_raw[i * piece : (i + 1) * piece, :].astype(F32)
            for k in range(kv):
                turned = jnp.transpose(wide[1, rows_of(k), :])
                v_turn[0, k, 0:width, i * cut : (i + 1) * cut] = turned.astype(BF16)

    def kv_sends(k):
        if pair == 1:
            return []
        return [
            remote(k_cut.at[0, k], k_cut.at[1, k], kv_send.at[k, 0], kv_recv.at[k, 0], twin),
            remote(v_turn.at[0, k], v_turn.at[1, k], kv_send.at[k, 1], kv_recv.at[k, 1], twin),
        ]

    def merge(one, two):
        top = jnp.maximum(one[0], two[0])
        a, b = jnp.exp2(one[0] - top), jnp.exp2(two[0] - top)
        return top, one[1] * a + two[1] * b, one[2] * a + two[2] * b

    buffers = ((scores_a, weights_a, top_a), (scores_b, weights_b, top_b))
    height = math.gcd(span, 256)

    def unit_scores(unit, at):
        block, k, tile = unit
        scores, _, tops = buffers[at]
        ask = qk[k, tile * columns : (tile + 1) * columns]
        top = None
        for j in range(span // height):
            part_of = slice(j * height, (j + 1) * height)
            x = dot_t(k_cut[block, k, part_of], ask)
            scores[part_of] = x
            x = jnp.max(x.reshape(height // 8, 8, columns), axis=0)
            top = x if top is None else jnp.maximum(top, x)
        tops[...] = jnp.broadcast_to(jnp.max(top, axis=0, keepdims=True), (8, columns))

    def unit_sums(unit, at):
        block, k, tile = unit
        scores, weights, tops = buffers[at]
        for j in range(span // height):
            part_of = slice(j * height, (j + 1) * height)
            x = scores[part_of].reshape(height // 8, 8, columns)
            x = jnp.exp2((x - tops[...][None]) * factor)
            weights[part_of] = x.reshape(height, columns).astype(BF16)
        out = jnp.dot(v_turn[block, k], weights[...], preferred_element_type=F32)
        top = tops[...] * factor
        to = slice(tile * columns, (tile + 1) * columns)
        if block > 0:
            old = top_all[k, :, to]
            new = jnp.maximum(old, top)
            a, b = jnp.exp2(old - new), jnp.exp2(top - new)
            out = acc_all[k, :, to] * a[0:1] + out * b[0:1]
            top = new
        if block < blocks - 1:
            acc_all[k, :, to] = out
            top_all[k, :, to] = top
            return
        row = lax.broadcasted_iota(jnp.int32, (8, LANES), 0)
        for c in range(columns // LANES):
            at_c = tile * columns + c * LANES
            here = slice(c * LANES, (c + 1) * LANES)
            slot, within = at_c // flat, at_c % flat
            if slot == 0:
                acc_all[k, :, at_c : at_c + LANES] = out[:, here]
                top_all[k, :, at_c : at_c + LANES] = top[:, here]
            else:
                into = slice(within, within + LANES)
                x = out[0:width, here]
                most = jnp.max(jnp.max(jnp.abs(x).reshape(width // 8, 8, LANES), axis=0), axis=0, keepdims=True)
                most = jnp.maximum(most, 1e-33)
                code = jnp.round(x * (CODES / most)).astype(jnp.int32)
                part[slot - 1, k, :, into] = code.astype(jnp.int16)
                stat = jnp.where(row == 1, top[:, here], most * (1.0 / CODES))
                part_stat[slot - 1, k, :, into] = jnp.where(row == 0, out[width : width + 8, here], stat)

    def partial_copies(t, k, i):
        at = slice(row_pieces[i][0] * group, row_pieces[i][1] * group)
        return [
            remote(
                src.at[t, k, :, at], dst.at[t, k, :, at], p_send.at[t, k, i, j], p_recv.at[t, k, i, j], backs[t]
            )
            for j, (src, dst) in enumerate(((part, got), (part_stat, got_stat)))
        ]

    split_at = (tiles - 1) * tile_rows * group // LANES

    def finals(lo, hi):
        per = LANES // group
        for c in range(lo, hi):
            at = slice(c * LANES, (c + 1) * LANES)
            done = []
            for k in range(kv):
                terms = (
                    top_all[k, 0:1, at],
                    acc_all[k, 0:width, at],
                    acc_all[k, width : width + 1, at],
                )
                for t in range(chips - 1):
                    terms = merge(
                        terms,
                        (
                            got_stat[t, k, 1:2, at],
                            got[t, k, :, at].astype(jnp.int32).astype(F32) * got_stat[t, k, 2:3, at],
                            got_stat[t, k, 0:1, at],
                        ),
                    )
                terms = merge(
                    (upright(terms[0]), jnp.transpose(terms[1]), upright(terms[2])),
                    (suf_top[k, at, :], suf_acc[k, at, :], suf_sum[k, at, :]),
                )
                done.append((terms[1] / terms[2]).reshape(per, 1, group, width))
            joined = jnp.concatenate(done, axis=1).reshape(per, heads, width)
            out_ref[c * per : (c + 1) * per] = joined.astype(BF16)

    def collect():
        for k in range(kv):
            for t in range(chips - 1):
                for i in range(len(row_pieces)):
                    for copy in partial_copies(t, k, i):
                        copy.wait_recv()
        finals(0, split_at)

    def run_units(steps):
        counts = {unit_scores: 0, suffix_scores: 0}
        ready_steps = []
        for before, first, second, unit, after in steps:
            ready_steps.append((before, first, second, unit, counts[first] % 2, after))
            counts[first] += 1
        for i, (before, first, second, unit, at, after) in enumerate(ready_steps):
            if i == 0:
                before()
                first(unit, at)
                kv_copies[1].wait()
                len_copy.wait()
            if i + 1 < len(ready_steps):
                before_next, first_next, _, unit_next, at_next, _ = ready_steps[i + 1]
                before_next()
                first_next(unit_next, at_next)
            if i == 0:
                settle()
            if i + 1 == len(ready_steps):
                collect()
            second(unit, at)
            after()

    def nop():
        pass

    asks, nears, fars = (ask_a, ask_b), (near_a, near_b), (far_a, far_b)
    half = slots // 2
    lane = lax.broadcasted_iota(jnp.int32, (8, LANES), 1)
    sublane = lax.broadcasted_iota(jnp.int32, (8, LANES), 0)
    same_head = sublane % kv == lane % heads // group
    diagonal = lax.broadcasted_iota(jnp.int32, (LANES, LANES), 0) == lax.broadcasted_iota(
        jnp.int32, (LANES, LANES), 1
    )

    def upright(row):
        wide_row = jnp.broadcast_to(row, (LANES, LANES))
        return jnp.sum(jnp.where(diagonal, wide_row, 0.0), axis=1, keepdims=True)

    def turn_queries():
        turned = jnp.transpose(q_raw[...].astype(F32).reshape(rows * heads, width)).astype(BF16)
        for tile in range(tiles):
            q_turn[tile] = turned[:, tile * LANES : (tile + 1) * LANES]

    def suffix_scores(tile, at):
        r0 = tile * tile_rows
        ask, (near, far) = asks[at], (nears[at], fars[at])
        turned = q_turn[tile]
        row_of = lax.broadcasted_iota(jnp.int32, (width, LANES), 1) // heads
        limit = jnp.zeros((8, LANES), jnp.int32)
        for r in range(tile_rows):
            mine = jnp.where(row_of == r, turned, jnp.zeros_like(turned))
            ask[2 * r * width : (2 * r + 1) * width, 0:LANES] = mine
            ask[(2 * r + 1) * width : (2 * r + 2) * width, LANES : 2 * LANES] = mine
            limit = jnp.where(lane // heads == r, len_ref[r0 + r] * kv, limit)
        limit = jnp.where(same_head, limit, -1)
        keys = jnp.concatenate(
            [sk[r0 + r, i * half : (i + 1) * half] for r in range(tile_rows) for i in range(2)], axis=1
        )
        both = jnp.dot(keys, ask[...], preferred_element_type=F32).reshape(half // 8, 8, 2 * LANES)
        slot = sublane[None] + 8 * lax.broadcasted_iota(jnp.int32, (half // 8, 8, LANES), 0)
        top = None
        for i in range(2):
            x = jnp.where(
                slot < (limit - i * half)[None], both[:, :, i * LANES : (i + 1) * LANES], MASKED
            )
            near[i] = x
            x = jnp.max(x, axis=0)
            top = x if top is None else jnp.maximum(top, x)
        far[...] = jnp.broadcast_to(jnp.max(top, axis=0, keepdims=True), (8, LANES))

    def suffix_sums(tile, at):
        r0 = tile * tile_rows
        near, far = nears[at], fars[at]
        total, parts = None, []
        for i in range(2):
            x = jnp.exp2((near[i] - far[...][None]) * factor).reshape(half, LANES).astype(BF16)
            y = jnp.sum(x.astype(F32).reshape(half // 8, 8, LANES), axis=0)
            total = y if total is None else total + y
            parts.append(jnp.transpose(x))
        weights = jnp.concatenate(parts, axis=1)
        total = jnp.sum(total, axis=0, keepdims=True)
        top = jnp.broadcast_to(upright(far[0:1] * factor), (LANES, width))
        total = jnp.broadcast_to(upright(total), (LANES, width))
        for r in range(tile_rows):
            acc = jnp.dot(weights[r * heads : (r + 1) * heads], sv[r0 + r], preferred_element_type=F32)
            to = slice((r0 + r) * group, (r0 + r + 1) * group)
            for k in range(kv):
                here = slice(r * heads + k * group, r * heads + (k + 1) * group)
                suf_acc[k, to, :] = acc[k * group : (k + 1) * group]
                suf_top[k, to, :] = top[here]
                suf_sum[k, to, :] = total[here]

    all_tiles = chips * flat // columns
    near = flat // columns

    def send_queries():
        if greeted:
            pl.semaphore_wait(barrier, len(greeted))
        for t in range(chips - 1):
            q_sends[t][0].start()

    def send_more_queries():
        for k in range(1, kv):
            for t in range(chips - 1):
                q_sends[t][k].start()

    def send_keys():
        for k in range(kv):
            for copy in kv_sends(k)[:1]:
                copy.start()

    def settle():
        turn_values()
        for k in range(kv):
            for copy in kv_sends(k)[1:]:
                copy.start()
        turn_queries()
        for ask in asks:
            ask[...] = jnp.zeros(ask.shape, BF16)

    q_copy.wait()
    split_queries()
    send_queries()
    kv_copies[0].wait()
    split_keys()
    send_keys()

    early = tiles // 3
    near_tiles = flat // columns
    all_tiles = chips * flat // columns
    waited = set()

    def ready(block, k, tile):
        def go():
            for t in range(chips - 1):
                if (t + 1) * flat < (tile + 1) * columns and ("q", t, k) not in waited:
                    waited.add(("q", t, k))
                    q_sends[t][k].wait_recv()
                    join_queries(t, k)
            if block > 0 and "kv" not in waited:
                waited.add("kv")
                for each in range(kv):
                    for copy in kv_sends(each):
                        copy.wait_recv()

        return go

    finished = set()

    def finish(block, k, tile):
        def go():
            if block < blocks - 1:
                return
            finished.update((k, at) for at in range(tile * columns, (tile + 1) * columns, LANES))
            for t in range(chips - 1):
                for i, (lo, hi) in enumerate(row_pieces):
                    begin, end = (t + 1) * flat + lo * group, (t + 1) * flat + hi * group
                    done = all((k, at) in finished for at in range(begin, end, LANES))
                    if done and ("p", t, k, i) not in waited:
                        waited.add(("p", t, k, i))
                        for copy in partial_copies(t, k, i):
                            copy.start()
                        if t == chips - 2:
                            take_suffixes()

        return go

    def documents(order):
        return [
            (ready(*unit), unit_scores, unit_sums, unit, finish(*unit)) for unit in order
        ]

    def arrived(tiles_of):
        def go():
            for tile in tiles_of:
                for copy in suffix_copies(tile):
                    copy.wait()
                if tile == 0:
                    send_more_queries()

        return go

    def take_suffixes():
        if "rest" not in waited:
            waited.add("rest")
            arrived(range(early, tiles))()

    def suffixes(tiles_of):
        return [
            (arrived([tile]) if tile < early else take_suffixes, suffix_scores, suffix_sums, tile, nop)
            for tile in tiles_of
        ]

    own_first = documents([(0, k, tile) for tile in range(near_tiles) for k in range(kv)])
    own_rest = documents(
        [(block, k, tile) for block in range(1, blocks) for tile in range(near_tiles) for k in range(kv)]
    )
    others = documents(
        [
            (block, k, tile)
            for k in range(kv)
            for tile in range(near_tiles, all_tiles)
            for block in range(blocks)
        ]
    )
    run_units(
        own_first
        + suffixes(range(early))
        + others
        + own_rest
        + suffixes(range(early, tiles))
    )

    finals(split_at, flat // LANES)
    for copies in q_sends:
        for copy in copies:
            copy.wait_send()
    for k in range(kv):
        for copy in kv_sends(k):
            copy.wait_send()
        for t in range(chips - 1):
            for i in range(len(row_pieces)):
                for copy in partial_copies(t, k, i):
                    copy.wait_send()


def shards(n_ctx, queries, prefix_keys, prefix_values, suffix_keys, suffix_values, lengths):
    rows, heads, width = queries.shape
    positions, kv, _ = prefix_keys.shape
    slots = suffix_keys.shape[1] * kv
    flat = rows * (heads // kv)
    pair = 2 if n_ctx % 2 == 0 else 1
    others = max(1, n_ctx // pair - 1)
    tile_rows = LANES // heads
    tiles = rows // tile_rows
    columns = math.gcd(n_ctx // pair * flat, 256)
    tall = width + 16
    piece = math.gcd(positions * kv, 1024)
    anywhere = pl.BlockSpec(memory_space=pl.ANY)
    vmem = pltpu.VMEM
    dma = pltpu.SemaphoreType.DMA
    call = pl.pallas_call(
        functools.partial(kernel, n_ctx, tile_rows),
        out_shape=jax.ShapeDtypeStruct((rows, heads, width), BF16),
        in_specs=[anywhere] * 6,
        out_specs=pl.BlockSpec(memory_space=vmem),
        scratch_shapes=[
            pltpu.SMEM((rows,), jnp.int32),
            vmem((rows, heads, width), BF16),
            vmem((others, kv, rows, heads // kv, width), BF16),
            vmem((kv, n_ctx // pair * flat, width), BF16),
            vmem((positions * kv, width), BF16),
            vmem((positions * kv, width), BF16),
            vmem((pair, kv, positions, width), BF16),
            vmem((pair, kv, tall, positions), BF16),
            vmem((2, piece, width), F32),
            vmem((rows, slots, width), BF16),
            vmem((rows, slots, width), BF16),
            vmem((positions, columns), F32),
            vmem((positions, columns), F32),
            vmem((positions, columns), BF16),
            vmem((positions, columns), BF16),
            vmem((8, columns), F32),
            vmem((8, columns), F32),
            vmem((2 * tile_rows * width, 2 * LANES), BF16),
            vmem((2 * tile_rows * width, 2 * LANES), BF16),
            vmem((2, slots // 16, 8, LANES), F32),
            vmem((2, slots // 16, 8, LANES), F32),
            vmem((8, LANES), F32),
            vmem((8, LANES), F32),
            vmem((kv, tall, n_ctx // pair * flat), F32),
            vmem((kv, 8, n_ctx // pair * flat), F32),
            vmem((others, kv, width, flat), jnp.int16),
            vmem((others, kv, width, flat), jnp.int16),
            vmem((others, kv, 8, flat), F32),
            vmem((others, kv, 8, flat), F32),
        ]
        + [vmem((tiles, width, LANES), BF16)]
        + [vmem((kv, flat, width), F32)] * 3
        + [
            dma,
            dma,
            dma((2,)),
            dma((tiles, 2)),
            dma((others, kv)),
            dma((others, kv)),
            dma((kv, 2)),
            dma((kv, 2)),
            dma((others, kv, 2, 2)),
            dma((others, kv, 2, 2)),
        ],
        compiler_params=pltpu.CompilerParams(
            collective_id=0, has_side_effects=True, vmem_limit_bytes=52 * 1024 * 1024
        ),
    )
    operands = (
        lengths,
        queries,
        prefix_keys.reshape(positions * kv, width),
        prefix_values.reshape(positions * kv, width),
        suffix_keys.reshape(rows, slots, width),
        suffix_values.reshape(rows, slots, width),
    )
    return call(*(pltpu.with_memory_space_constraint(x, pltpu.HBM) for x in operands))


def solution(mesh):
    placed = (
        P(("groups", "ctx"), "head", None),
        P(("groups", "ctx"), "head", None),
        P(("groups", "ctx"), "head", None),
        P(("groups", "ctx"), None, "head", None),
        P(("groups", "ctx"), None, "head", None),
        P(("groups", "ctx")),
    )
    return jax.shard_map(
        functools.partial(shards, mesh.shape["ctx"]),
        mesh=mesh,
        in_specs=placed,
        out_specs=P(("groups", "ctx"), "head", None),
        check_vma=False,
    )
```

```python
import functools
import math

import jax
import jax.numpy as jnp
from jax import lax
from jax.experimental import pallas as pl
from jax.experimental.pallas import tpu as pltpu
from jax.sharding import PartitionSpec as P

F32 = jnp.float32
BF16 = jnp.bfloat16
MASKED = -1e30
LANES = 128
CODES = 32767.0


def dot_t(a, b):
    return lax.dot_general(a, b, (((1,), (1,)), ((), ())), preferred_element_type=F32)


def kernel(
    n_ctx, tile_rows,
    len_hbm, q_hbm, pk_hbm, pv_hbm, sk_hbm, sv_hbm, out_ref,
    len_ref,
    q_raw, q_far, qk, k_raw, v_raw, k_cut, v_turn, wide, sk, sv,
    scores_a, scores_b, weights_a, weights_b, top_a, top_b,
    ask_a, ask_b, near_a, near_b, far_a, far_b, acc_all, top_all, part, got, part_stat, got_stat, q_turn, suf_acc, suf_top, suf_sum,
    len_sem, q_sem, kv_sem, suf_sem, q_send, q_recv, kv_send, kv_recv, p_send, p_recv,
):
    rows, heads, width = q_hbm.shape
    kv = k_cut.shape[1]
    group = heads // kv
    flat = rows * group
    pair = 2 if n_ctx % 2 == 0 else 1
    chips = n_ctx // pair
    blocks = pair
    factor = width ** (-0.5) * math.log2(math.e)
    tiles = rows // tile_rows
    slots = sk.shape[1]
    span = k_cut.shape[2]
    tall = v_turn.shape[2]
    columns = scores_a.shape[1]
    me = lax.axis_index("ctx")
    chip, core = me // pair, me % pair

    def device(chip_at, core_at):
        return {"ctx": chip_at * pair + core_at}

    def remote(src, dst, send, recv, target):
        return pltpu.make_async_remote_copy(
            src_ref=src, dst_ref=dst, send_sem=send, recv_sem=recv,
            device_id=target, device_id_type=pl.DeviceIdType.MESH,
        )

    q_copy = pltpu.make_async_copy(q_hbm, q_raw, q_sem)
    q_copy.start()
    kv_copies = [
        pltpu.make_async_copy(pk_hbm, k_raw, kv_sem.at[0]),
        pltpu.make_async_copy(pv_hbm, v_raw, kv_sem.at[1]),
    ]
    for copy in kv_copies:
        copy.start()
    len_copy = pltpu.make_async_copy(len_hbm, len_ref, len_sem)
    len_copy.start()

    def suffix_copies(tile):
        at = pl.ds(tile * tile_rows, tile_rows)
        return (
            pltpu.make_async_copy(sk_hbm.at[at], sk.at[at], suf_sem.at[tile, 0]),
            pltpu.make_async_copy(sv_hbm.at[at], sv.at[at], suf_sem.at[tile, 1]),
        )

    partners = [device(lax.rem(chip + t, chips), core) for t in range(1, chips)]
    backs = [device(lax.rem(chip - t + chips, chips), core) for t in range(1, chips)]
    twin = device(chip, pair - 1 - core)
    greeted = partners + ([twin] if pair == 2 else [])
    barrier = pltpu.get_barrier_semaphore() if greeted else None
    for target in greeted:
        pl.semaphore_signal(
            barrier, inc=1, device_id=target, device_id_type=pl.DeviceIdType.MESH
        )

    row_pieces = [(0, rows)]
    q_sends = [
        [
            remote(
                q_hbm.at[:, k * group : (k + 1) * group], q_far.at[t, k],
                q_send.at[t, k], q_recv.at[t, k], partners[t],
            )
            for k in range(kv)
        ]
        for t in range(chips - 1)
    ]

    def start_tile(tile, carry):
        for copy in suffix_copies(tile):
            copy.start()
        return carry

    lax.fori_loop(0, tiles, start_tile, 0)

    def split_queries():
        wide_q = q_raw[...].astype(F32).reshape(rows, kv, group, width)
        for k in range(kv):
            qk[k, 0:flat] = wide_q[:, k].reshape(flat, width).astype(BF16)

    def join_queries(t, k):
        far_q = q_far[t, k].astype(F32).reshape(flat, width).astype(BF16)
        qk[k, (t + 1) * flat : (t + 2) * flat] = far_q

    piece = wide.shape[1]
    cut = piece // kv

    def rows_of(k):
        return pl.ds(k, cut, stride=kv) if kv > 1 else pl.ds(0, piece)

    def split_keys():
        def step(i, carry):
            wide[0] = k_raw[pl.ds(pl.multiple_of(i * piece, piece), piece), :].astype(F32)
            to = pl.ds(pl.multiple_of(i * cut, cut), cut)
            for k in range(kv):
                k_cut[0, k, to, :] = wide[0, rows_of(k), :].astype(BF16)
            return carry

        lax.fori_loop(0, span * kv // piece, step, 0)

    def turn_values():
        ones = (lax.broadcasted_iota(jnp.int32, (tall - width, span), 0) == 0).astype(F32)
        for k in range(kv):
            v_turn[0, k, width:tall, :] = ones.astype(BF16)
        for i in range(span * kv // piece):
            wide[1] = v_raw[i * piece : (i + 1) * piece, :].astype(F32)
            for k in range(kv):
                turned = jnp.transpose(wide[1, rows_of(k), :])
                v_turn[0, k, 0:width, i * cut : (i + 1) * cut] = turned.astype(BF16)

    def kv_sends(k):
        if pair == 1:
            return []
        return [
            remote(k_cut.at[0, k], k_cut.at[1, k], kv_send.at[k, 0], kv_recv.at[k, 0], twin),
            remote(v_turn.at[0, k], v_turn.at[1, k], kv_send.at[k, 1], kv_recv.at[k, 1], twin),
        ]

    def merge(one, two):
        top = jnp.maximum(one[0], two[0])
        a, b = jnp.exp2(one[0] - top), jnp.exp2(two[0] - top)
        return top, one[1] * a + two[1] * b, one[2] * a + two[2] * b

    buffers = ((scores_a, weights_a, top_a), (scores_b, weights_b, top_b))
    height = math.gcd(span, 256)

    def unit_scores(unit, at):
        block, k, tile = unit
        scores, _, tops = buffers[at]
        ask = qk[k, tile * columns : (tile + 1) * columns]
        top = None
        for j in range(span // height):
            part_of = slice(j * height, (j + 1) * height)
            x = dot_t(k_cut[block, k, part_of], ask)
            scores[part_of] = x
            x = jnp.max(x.reshape(height // 8, 8, columns), axis=0)
            top = x if top is None else jnp.maximum(top, x)
        tops[...] = jnp.broadcast_to(jnp.max(top, axis=0, keepdims=True), (8, columns))

    def unit_sums(unit, at):
        block, k, tile = unit
        scores, weights, tops = buffers[at]
        for j in range(span // height):
            part_of = slice(j * height, (j + 1) * height)
            x = scores[part_of].reshape(height // 8, 8, columns)
            x = jnp.exp2((x - tops[...][None]) * factor)
            weights[part_of] = x.reshape(height, columns).astype(BF16)
        out = jnp.dot(v_turn[block, k], weights[...], preferred_element_type=F32)
        top = tops[...] * factor
        to = slice(tile * columns, (tile + 1) * columns)
        if block > 0:
            old = top_all[k, :, to]
            new = jnp.maximum(old, top)
            a, b = jnp.exp2(old - new), jnp.exp2(top - new)
            out = acc_all[k, :, to] * a[0:1] + out * b[0:1]
            top = new
        if block < blocks - 1:
            acc_all[k, :, to] = out
            top_all[k, :, to] = top
            return
        row = lax.broadcasted_iota(jnp.int32, (8, LANES), 0)
        for c in range(columns // LANES):
            at_c = tile * columns + c * LANES
            here = slice(c * LANES, (c + 1) * LANES)
            slot, within = at_c // flat, at_c % flat
            if slot == 0:
                acc_all[k, :, at_c : at_c + LANES] = out[:, here]
                top_all[k, :, at_c : at_c + LANES] = top[:, here]
            else:
                into = slice(within, within + LANES)
                x = out[0:width, here]
                most = jnp.max(jnp.max(jnp.abs(x).reshape(width // 8, 8, LANES), axis=0), axis=0, keepdims=True)
                most = jnp.maximum(most, 1e-33)
                code = jnp.round(x * (CODES / most)).astype(jnp.int32)
                part[slot - 1, k, :, into] = code.astype(jnp.int16)
                stat = jnp.where(row == 1, top[:, here], most * (1.0 / CODES))
                part_stat[slot - 1, k, :, into] = jnp.where(row == 0, out[width : width + 8, here], stat)

    def partial_copies(t, k, i):
        at = slice(row_pieces[i][0] * group, row_pieces[i][1] * group)
        return [
            remote(
                src.at[t, k, :, at], dst.at[t, k, :, at], p_send.at[t, k, i, j], p_recv.at[t, k, i, j], backs[t]
            )
            for j, (src, dst) in enumerate(((part, got), (part_stat, got_stat)))
        ]

    split_at = (tiles - 1) * tile_rows * group // LANES

    def finals(lo, hi):
        per = LANES // group
        for c in range(lo, hi):
            at = slice(c * LANES, (c + 1) * LANES)
            done = []
            for k in range(kv):
                terms = (
                    top_all[k, 0:1, at],
                    acc_all[k, 0:width, at],
                    acc_all[k, width : width + 1, at],
                )
                for t in range(chips - 1):
                    terms = merge(
                        terms,
                        (
                            got_stat[t, k, 1:2, at],
                            got[t, k, :, at].astype(jnp.int32).astype(F32) * got_stat[t, k, 2:3, at],
                            got_stat[t, k, 0:1, at],
                        ),
                    )
                terms = merge(
                    (upright(terms[0]), jnp.transpose(terms[1]), upright(terms[2])),
                    (suf_top[k, at, :], suf_acc[k, at, :], suf_sum[k, at, :]),
                )
                done.append((terms[1] / terms[2]).reshape(per, 1, group, width))
            joined = jnp.concatenate(done, axis=1).reshape(per, heads, width)
            out_ref[c * per : (c + 1) * per] = joined.astype(BF16)

    def collect():
        for k in range(kv):
            for t in range(chips - 1):
                for i in range(len(row_pieces)):
                    for copy in partial_copies(t, k, i):
                        copy.wait_recv()
        finals(0, split_at)

    def run_units(steps):
        counts = {unit_scores: 0, suffix_scores: 0}
        ready_steps = []
        for before, first, second, unit, after in steps:
            ready_steps.append((before, first, second, unit, counts[first] % 2, after))
            counts[first] += 1
        for i, (before, first, second, unit, at, after) in enumerate(ready_steps):
            if i == 0:
                before()
                first(unit, at)
                kv_copies[1].wait()
                len_copy.wait()
            if i + 1 < len(ready_steps):
                before_next, first_next, _, unit_next, at_next, _ = ready_steps[i + 1]
                before_next()
                first_next(unit_next, at_next)
            if i == 0:
                settle()
            if i + 1 == len(ready_steps):
                collect()
            second(unit, at)
            after()

    def nop():
        pass

    asks, nears, fars = (ask_a, ask_b), (near_a, near_b), (far_a, far_b)
    half = slots // 2
    lane = lax.broadcasted_iota(jnp.int32, (8, LANES), 1)
    sublane = lax.broadcasted_iota(jnp.int32, (8, LANES), 0)
    same_head = sublane % kv == lane % heads // group
    diagonal = lax.broadcasted_iota(jnp.int32, (LANES, LANES), 0) == lax.broadcasted_iota(
        jnp.int32, (LANES, LANES), 1
    )

    def upright(row):
        wide_row = jnp.broadcast_to(row, (LANES, LANES))
        return jnp.sum(jnp.where(diagonal, wide_row, 0.0), axis=1, keepdims=True)

    def turn_queries():
        turned = jnp.transpose(q_raw[...].astype(F32).reshape(rows * heads, width)).astype(BF16)
        for tile in range(tiles):
            q_turn[tile] = turned[:, tile * LANES : (tile + 1) * LANES]

    def suffix_scores(tile, at):
        r0 = tile * tile_rows
        ask, (near, far) = asks[at], (nears[at], fars[at])
        turned = q_turn[tile]
        row_of = lax.broadcasted_iota(jnp.int32, (width, LANES), 1) // heads
        limit = jnp.zeros((8, LANES), jnp.int32)
        for r in range(tile_rows):
            mine = jnp.where(row_of == r, turned, jnp.zeros_like(turned))
            ask[2 * r * width : (2 * r + 1) * width, 0:LANES] = mine
            ask[(2 * r + 1) * width : (2 * r + 2) * width, LANES : 2 * LANES] = mine
            limit = jnp.where(lane // heads == r, len_ref[r0 + r] * kv, limit)
        limit = jnp.where(same_head, limit, -1)
        keys = jnp.concatenate(
            [sk[r0 + r, i * half : (i + 1) * half] for r in range(tile_rows) for i in range(2)], axis=1
        )
        both = jnp.dot(keys, ask[...], preferred_element_type=F32).reshape(half // 8, 8, 2 * LANES)
        slot = sublane[None] + 8 * lax.broadcasted_iota(jnp.int32, (half // 8, 8, LANES), 0)
        top = None
        for i in range(2):
            x = jnp.where(
                slot < (limit - i * half)[None], both[:, :, i * LANES : (i + 1) * LANES], MASKED
            )
            near[i] = x
            x = jnp.max(x, axis=0)
            top = x if top is None else jnp.maximum(top, x)
        far[...] = jnp.broadcast_to(jnp.max(top, axis=0, keepdims=True), (8, LANES))

    def suffix_sums(tile, at):
        r0 = tile * tile_rows
        near, far = nears[at], fars[at]
        total, parts = None, []
        for i in range(2):
            x = jnp.exp2((near[i] - far[...][None]) * factor).reshape(half, LANES).astype(BF16)
            y = jnp.sum(x.astype(F32).reshape(half // 8, 8, LANES), axis=0)
            total = y if total is None else total + y
            parts.append(jnp.transpose(x))
        weights = jnp.concatenate(parts, axis=1)
        total = jnp.sum(total, axis=0, keepdims=True)
        top = jnp.broadcast_to(upright(far[0:1] * factor), (LANES, width))
        total = jnp.broadcast_to(upright(total), (LANES, width))
        for r in range(tile_rows):
            acc = jnp.dot(weights[r * heads : (r + 1) * heads], sv[r0 + r], preferred_element_type=F32)
            to = slice((r0 + r) * group, (r0 + r + 1) * group)
            for k in range(kv):
                here = slice(r * heads + k * group, r * heads + (k + 1) * group)
                suf_acc[k, to, :] = acc[k * group : (k + 1) * group]
                suf_top[k, to, :] = top[here]
                suf_sum[k, to, :] = total[here]

    all_tiles = chips * flat // columns
    near = flat // columns

    def send_queries():
        if greeted:
            pl.semaphore_wait(barrier, len(greeted))
        for t in range(chips - 1):
            q_sends[t][0].start()

    def send_more_queries():
        for k in range(1, kv):
            for t in range(chips - 1):
                q_sends[t][k].start()

    def send_keys():
        for k in range(kv):
            for copy in kv_sends(k)[:1]:
                copy.start()

    def settle():
        turn_values()
        for k in range(kv):
            for copy in kv_sends(k)[1:]:
                copy.start()
        turn_queries()
        for ask in asks:
            ask[...] = jnp.zeros(ask.shape, BF16)

    send_queries()
    q_copy.wait()
    split_queries()
    kv_copies[0].wait()
    split_keys()
    send_keys()

    early = tiles // 3
    near_tiles = flat // columns
    all_tiles = chips * flat // columns
    waited = set()

    def ready(block, k, tile):
        def go():
            for t in range(chips - 1):
                if (t + 1) * flat < (tile + 1) * columns and ("q", t, k) not in waited:
                    waited.add(("q", t, k))
                    q_sends[t][k].wait_recv()
                    join_queries(t, k)
            if block > 0 and "kv" not in waited:
                waited.add("kv")
                for each in range(kv):
                    for copy in kv_sends(each):
                        copy.wait_recv()

        return go

    finished = set()

    def finish(block, k, tile):
        def go():
            if block < blocks - 1:
                return
            finished.update((k, at) for at in range(tile * columns, (tile + 1) * columns, LANES))
            for t in range(chips - 1):
                for i, (lo, hi) in enumerate(row_pieces):
                    begin, end = (t + 1) * flat + lo * group, (t + 1) * flat + hi * group
                    done = all((k, at) in finished for at in range(begin, end, LANES))
                    if done and ("p", t, k, i) not in waited:
                        waited.add(("p", t, k, i))
                        for copy in partial_copies(t, k, i):
                            copy.start()
                        if t == chips - 2:
                            take_suffixes()

        return go

    def documents(order):
        return [
            (ready(*unit), unit_scores, unit_sums, unit, finish(*unit)) for unit in order
        ]

    def arrived(tiles_of):
        def go():
            for tile in tiles_of:
                for copy in suffix_copies(tile):
                    copy.wait()
                if tile == 0:
                    send_more_queries()

        return go

    def take_suffixes():
        if "rest" not in waited:
            waited.add("rest")
            arrived(range(early, tiles))()

    def suffixes(tiles_of):
        return [
            (arrived([tile]) if tile < early else take_suffixes, suffix_scores, suffix_sums, tile, nop)
            for tile in tiles_of
        ]

    own_first = documents([(0, k, tile) for tile in range(near_tiles) for k in range(kv)])
    own_rest = documents(
        [(block, k, tile) for block in range(1, blocks) for tile in range(near_tiles) for k in range(kv)]
    )
    others = documents(
        [
            (block, k, tile)
            for k in range(kv)
            for tile in range(near_tiles, all_tiles)
            for block in range(blocks)
        ]
    )
    run_units(
        own_first
        + suffixes(range(early))
        + others
        + own_rest
        + suffixes(range(early, tiles))
    )

    finals(split_at, flat // LANES)
    for copies in q_sends:
        for copy in copies:
            copy.wait_send()
    for k in range(kv):
        for copy in kv_sends(k):
            copy.wait_send()
        for t in range(chips - 1):
            for i in range(len(row_pieces)):
                for copy in partial_copies(t, k, i):
                    copy.wait_send()


def shards(n_ctx, queries, prefix_keys, prefix_values, suffix_keys, suffix_values, lengths):
    rows, heads, width = queries.shape
    positions, kv, _ = prefix_keys.shape
    slots = suffix_keys.shape[1] * kv
    flat = rows * (heads // kv)
    pair = 2 if n_ctx % 2 == 0 else 1
    others = max(1, n_ctx // pair - 1)
    tile_rows = LANES // heads
    tiles = rows // tile_rows
    columns = math.gcd(n_ctx // pair * flat, 256)
    tall = width + 16
    piece = math.gcd(positions * kv, 1024)
    anywhere = pl.BlockSpec(memory_space=pl.ANY)
    vmem = pltpu.VMEM
    dma = pltpu.SemaphoreType.DMA
    call = pl.pallas_call(
        functools.partial(kernel, n_ctx, tile_rows),
        out_shape=jax.ShapeDtypeStruct((rows, heads, width), BF16),
        in_specs=[anywhere] * 6,
        out_specs=pl.BlockSpec(memory_space=vmem),
        scratch_shapes=[
            pltpu.SMEM((rows,), jnp.int32),
            vmem((rows, heads, width), BF16),
            vmem((others, kv, rows, heads // kv, width), BF16),
            vmem((kv, n_ctx // pair * flat, width), BF16),
            vmem((positions * kv, width), BF16),
            vmem((positions * kv, width), BF16),
            vmem((pair, kv, positions, width), BF16),
            vmem((pair, kv, tall, positions), BF16),
            vmem((2, piece, width), F32),
            vmem((rows, slots, width), BF16),
            vmem((rows, slots, width), BF16),
            vmem((positions, columns), F32),
            vmem((positions, columns), F32),
            vmem((positions, columns), BF16),
            vmem((positions, columns), BF16),
            vmem((8, columns), F32),
            vmem((8, columns), F32),
            vmem((2 * tile_rows * width, 2 * LANES), BF16),
            vmem((2 * tile_rows * width, 2 * LANES), BF16),
            vmem((2, slots // 16, 8, LANES), F32),
            vmem((2, slots // 16, 8, LANES), F32),
            vmem((8, LANES), F32),
            vmem((8, LANES), F32),
            vmem((kv, tall, n_ctx // pair * flat), F32),
            vmem((kv, 8, n_ctx // pair * flat), F32),
            vmem((others, kv, width, flat), jnp.int16),
            vmem((others, kv, width, flat), jnp.int16),
            vmem((others, kv, 8, flat), F32),
            vmem((others, kv, 8, flat), F32),
        ]
        + [vmem((tiles, width, LANES), BF16)]
        + [vmem((kv, flat, width), F32)] * 3
        + [
            dma,
            dma,
            dma((2,)),
            dma((tiles, 2)),
            dma((others, kv)),
            dma((others, kv)),
            dma((kv, 2)),
            dma((kv, 2)),
            dma((others, kv, 2, 2)),
            dma((others, kv, 2, 2)),
        ],
        compiler_params=pltpu.CompilerParams(
            collective_id=0, has_side_effects=True, vmem_limit_bytes=52 * 1024 * 1024
        ),
    )
    operands = (
        lengths,
        queries,
        prefix_keys.reshape(positions * kv, width),
        prefix_values.reshape(positions * kv, width),
        suffix_keys.reshape(rows, slots, width),
        suffix_values.reshape(rows, slots, width),
    )
    return call(*(pltpu.with_memory_space_constraint(x, pltpu.HBM) for x in operands))


def solution(mesh):
    placed = (
        P(("groups", "ctx"), "head", None),
        P(("groups", "ctx"), "head", None),
        P(("groups", "ctx"), "head", None),
        P(("groups", "ctx"), None, "head", None),
        P(("groups", "ctx"), None, "head", None),
        P(("groups", "ctx")),
    )
    return jax.shard_map(
        functools.partial(shards, mesh.shape["ctx"]),
        mesh=mesh,
        in_specs=placed,
        out_specs=P(("groups", "ctx"), "head", None),
        check_vma=False,
    )
```
